128 devices in a mesh: row: 16 (over x_lo, z, core), col: 8 (over y, x_hi).
Axes of the slice: x: 4 (x_hi: 2, x_lo: 2; x = x_hi * 2 + x_lo), y: 4, z: 4, core: 2. Of those that a mesh axis runs over, the one named last changes fastest.
Arguments:
- die_current: float32 [16, 2048, 2048], P(None, 'row', 'col')
- die_shunt: float32 [2048, 2048], P('row', 'col'), may hold values from 0.01 to 0.1
- pkg_current: float32 [16, 4096], P(None, ('row', 'col')), may hold values from -6 to 6
- pkg_matrix: float32 [4096, 4096], P('row', 'col'), as said below
- pkg_block_inv: float32 [128, 32, 32], P(('row', 'col')), as said below
- bump_node: int32 [4096], replicated, may hold values from 0 to 4194303, as said below
- bump_conductance: float32 [4096], replicated, may hold values from 0.5 to 4
Outputs:
- die_drop: float32 [16, 2048, 2048], P(None, 'row', 'col')
- package_drop: float32 [16, 4096], P(None, ('row', 'col'))
The draws below stay inside these ranges and needn't reach their ends.
Inputs may be any that keep to these rules, and one draw needn't show every extreme that they name: `bump_node`: bump b lies in lattice cell (b // 64, b % 64) of the die, the cells being 32 rows by 32 columns; the entry is row * 2048 + column, so no two bumps share a node. `pkg_matrix`: symmetric positive definite. `pkg_block_inv`: each block is symmetric positive definite.
All inputs are finite; a program needn't handle non-finite values.
Results may differ from the reference program's by a relative error of at most 0.0003.
Values sent between devices are 32-bit elements; how exact they have to be, the bound alone decides.
No kernel may reach another device: no remote copies, remote signals or barrier semaphores. Data moves between devices by JAX's collectives and lax.ppermute only.
A program may use at most 128 MiB of HBM per device.

```python
import math
import jax
import jax.numpy as jnp
from jax import lax

K = 16
NB = 4096
BUMP_C = 64
PB = 32
ITERS = 3
BUMP_R = 64
NX = 2048
NY = 2048


def draw_die_current(key, part):
    rows = jnp.arange(NX, dtype=jnp.float32) / NX
    cols = jnp.arange(NY, dtype=jnp.float32) / NY
    scale = (0.5 + 1.5 * rows)[:, None] * (0.7 + 0.7 * cols)[None, :]
    return jax.random.normal(jax.random.fold_in(key, 12), (K, NX, NY), jnp.float32) * scale


def draw_pkg_matrix(key, part):
    raw = jax.random.normal(jax.random.fold_in(key, 21), (NB, NB), jnp.float32)
    off = (raw + raw.T) / jnp.sqrt(2.0 * NB)
    diag = jax.random.uniform(jax.random.fold_in(key, 22), (NB,), jnp.float32, 4.0, 8.0)
    return off + jnp.diag(diag)


def draw_pkg_block_inv(key, part):
    count = NB // PB
    raw = jax.random.normal(jax.random.fold_in(key, 31), (count, PB, PB), jnp.float32)
    sym = (raw + jnp.swapaxes(raw, 1, 2)) / jnp.sqrt(2.0) * (0.05 / jnp.sqrt(1.0 * PB))
    diag = jax.random.uniform(jax.random.fold_in(key, 32), (count, PB), jnp.float32, 0.15, 0.35)
    return sym + diag[:, :, None] * jnp.eye(PB, dtype=jnp.float32)[None, :, :]


def draw_bump_node(key, part):
    cell_rows = NX // BUMP_R
    cell_cols = NY // BUMP_C
    row_off = jax.random.randint(jax.random.fold_in(key, 41), (NB,), 0, cell_rows)
    col_off = jax.random.randint(jax.random.fold_in(key, 42), (NB,), 0, cell_cols)
    ids = jnp.arange(NB, dtype=jnp.int32)
    grid_row = ids // BUMP_C * cell_rows + row_off
    grid_col = ids % BUMP_C * cell_cols + col_off
    return (grid_row * NY + grid_col).astype(jnp.int32)


def block_levels(own_key, shape, pieces, least, top_value):
    loudness = 1.0
    for position, parts in pieces:
        heights = jax.random.uniform(jax.random.fold_in(jax.random.fold_in(own_key, 6), position), (parts,), jnp.float32, least / len(pieces), top_value / len(pieces))
        loudness = loudness * jnp.repeat(jnp.exp(heights), shape[position] // parts).reshape((-1,) + (1,) * (len(shape) - 1 - position))
    return loudness


def normal_values(rng, dims, width, most, shards=(), kind=jnp.bfloat16):
    gain = block_levels(rng, dims, shards, -0.22, 0.18) if shards else 1.0
    entries = jax.random.normal(rng, dims, jnp.float32) * width * gain
    return jnp.minimum(jnp.maximum(entries, -most), most).astype(kind)


def setup_inputs(seed: int = 0) -> dict:
    key_list = jax.random.split(jax.random.key(seed), 8)
    die_current = draw_die_current(jax.random.fold_in(key_list[7], 71), 0)
    die_shunt = jnp.clip(jnp.exp(math.log(0.1) - 2.3025851 * jax.random.uniform(key_list[1], (NX, NY), jnp.float32) ** block_levels(key_list[1], (NX, NY), ((0, 16), (1, 8)), -0.2, 0.2)), 0.01, 0.1)
    pkg_current = normal_values(key_list[2], (K, NB), 1.0, 6.0, ((1, 128),), jnp.float32)
    pkg_matrix = draw_pkg_matrix(jax.random.fold_in(key_list[7], 71), 0)
    pkg_block_inv = draw_pkg_block_inv(jax.random.fold_in(key_list[7], 71), 0)
    bump_node = draw_bump_node(jax.random.fold_in(key_list[7], 71), 0)
    bump_conductance = jnp.clip(jnp.exp(jax.random.uniform(key_list[6], (NB,), jnp.float32, math.log(0.5), math.log(4.0))), 0.5, 4.0)
    return dict(die_current=die_current, die_shunt=die_shunt, pkg_current=pkg_current, pkg_matrix=pkg_matrix, pkg_block_inv=pkg_block_inv, bump_node=bump_node, bump_conductance=bump_conductance)


def laplace(field, shunt):
    padded = jnp.pad(field, ((0, 0), (1, 1), (1, 1)))
    beside_all = padded[:, 2:, 1:-1] + padded[:, :-2, 1:-1]
    beside_all = beside_all + padded[:, 1:-1, 2:] + padded[:, 1:-1, :-2]
    return (4.0 + shunt) * field - beside_all


def reference(die_current, die_shunt, pkg_current, pkg_matrix, pkg_block_inv, bump_node, bump_conductance):
    rows_b = (bump_node // NY).astype(jnp.int32)
    cols_b = (bump_node % NY).astype(jnp.int32)
    diag_die = (4.0 + die_shunt).at[rows_b, cols_b].add(bump_conductance)

    def apply_op(vd, vp):
        at_bumps = vd[:, rows_b, cols_b]
        die = laplace(vd, die_shunt).at[:, rows_b, cols_b].add(bump_conductance * (at_bumps - vp))
        prod = lax.dot_general(vp, pkg_matrix, (((1,), (1,)), ((), ())), precision=lax.Precision.HIGHEST)
        return die, prod + bump_conductance * (vp - at_bumps)

    def precond(rd, rp):
        blocks = rp.reshape(rp.shape[0], -1, PB)
        zp = jnp.einsum("bac,kbc->kba", pkg_block_inv, blocks, precision=lax.Precision.HIGHEST)
        return rd / diag_die, zp.reshape(rp.shape)

    def inner(ad, ap, bd, bp):
        return jnp.sum(ad * bd, axis=(1, 2)) + jnp.sum(ap * bp, axis=1)

    xd = jnp.zeros_like(die_current)
    xp = jnp.zeros_like(pkg_current)
    rd, rp = die_current, pkg_current
    zd, zp = precond(rd, rp)
    pd, pp = zd, zp
    rz = inner(rd, rp, zd, zp)
    for step in range(ITERS):
        qd, qp = apply_op(pd, pp)
        alpha = rz / inner(pd, pp, qd, qp)
        xd = xd + alpha[:, None, None] * pd
        xp = xp + alpha[:, None] * pp
        rd = rd - alpha[:, None, None] * qd
        rp = rp - alpha[:, None] * qp
        zd, zp = precond(rd, rp)
        fresh = inner(rd, rp, zd, zp)
        ratio = fresh / rz
        pd = zd + ratio[:, None, None] * pd
        pp = zp + ratio[:, None] * pp
        rz = fresh
    return xd, xp
```

```python
import functools

import jax
import jax.numpy as jnp
from jax import lax
from jax.experimental import pallas as pl
from jax.experimental.pallas import tpu as pltpu
from jax.sharding import Mesh
from jax.sharding import PartitionSpec as P

ROW = ("row_0", "row_1", "row_2")
COL = ("col_0", "col_1")
ROW_COL = ("row_0", "row_1", "row_2", "col_0", "col_1")

K = 16
TR, TC = 128, 256
ER, EC = 136, 384
CELL = 32
PLANES = K + 1
PAIRS = 9
HROWS = 56
OWN = 32
NB = 4096
HI = lax.Precision.HIGHEST


def iota(shape, dim):
    return lax.broadcasted_iota(jnp.int32, shape, dim)


def where_am_i():
    i = (lax.axis_index("row_0") * 4 + lax.axis_index("row_1")) * 2 + lax.axis_index("row_2")
    j = lax.axis_index("col_0") * 2 + lax.axis_index("col_1")
    return i, j


def dot_nt(a, b):
    return lax.dot_general(
        a, b, (((1,), (1,)), ((), ())), precision=HI, preferred_element_type=jnp.float32
    )


def dot_nn(a, b):
    return jnp.dot(a, b, precision=HI, preferred_element_type=jnp.float32)


def spread(j):
    group = iota((128, EC), 1) // CELL
    cell = jnp.where(group <= 8, 8 * j + group, jnp.where(group == 11, 8 * j - 1, -5))
    return (iota((128, EC), 0) % 64 == cell).astype(jnp.float32)


def lattice_chunk(l):
    return jnp.clip(l // 2, 0, NB // 128 - 1)


def extended_rows(parts):
    body = [jnp.broadcast_to(p, (CELL, EC)) for p in parts[1:5]]
    edge = jnp.where(iota((8, EC), 0) < 4, parts[5], parts[0])
    return jnp.concatenate(body + [edge], axis=0)


def padded(scr, x):
    scr[...] = jnp.zeros_like(scr)
    scr[:, 0 : x.shape[1]] = x
    return scr[...]


def pack(vp, vd):
    lane = iota((8, 128), 1)
    hi = pltpu.roll(vp[8:16], 32, 1)
    out = jnp.where(lane < 32, vp[0:8], hi)
    out = jnp.where(lane < 64, out, pltpu.roll(vd[0:8], 64, 1))
    return jnp.where(lane < 96, out, pltpu.roll(vd[8:16], 96, 1))


def gather_bumps(s_ref):
    at = iota((4 * TC, 128), 0)
    pick = (at // TC * 8 + at % TC // CELL == iota((4 * TC, 128), 1)).astype(jnp.float32)
    return dot_nn(s_ref[...], pick)


def down_cells(s_ref, k, z):
    for lr in range(4):
        rows = z[CELL * lr : CELL * (lr + 1)]
        s_ref[pl.ds(k, 1), TC * lr : TC * (lr + 1)] = jnp.sum(rows, axis=0, keepdims=True)


def fill(msg_ref, pay):
    def one(d, c):
        msg_ref[d] = pay
        return c

    lax.fori_loop(0, msg_ref.shape[0], one, 0, unroll=8)


def first_kernel(
    b_ref, sh_ref, bp_ref, p_ref, m_ref, node_ref, cond_ref,
    msg1_ref, msg0_ref, cm_ref, edge_ref, v0p_ref,
    a_ref, s_ref, pad_ref, z_ref,
):
    i, j = where_am_i()
    for t in range(4):
        for d in range(8):
            msg1_ref[d, 32 * t : 32 * (t + 1), :] = p_ref[32 * d : 32 * (d + 1), 128 * t : 128 * (t + 1)]
    lane = iota((TR, 128), 1)
    z = jnp.zeros((TR, 128), jnp.float32)
    for k in range(PLANES):
        lo = b_ref[k, :, 0:128] if k < K else sh_ref[:, 0:128]
        up = b_ref[k, :, 128:256] if k < K else sh_ref[:, 128:256]
        lo = pltpu.roll(lo, 3 * k, 1) if k else lo
        up = pltpu.roll(up, (64 + 3 * k - 125) % 128, 1)
        z = jnp.where((lane >= 3 * k) & (lane < 3 * k + 3), lo, z)
        z = jnp.where((lane >= 64 + 3 * k) & (lane < 67 + 3 * k), up, z)
    z_ref[...] = z.T

    @pl.when(j > 0)
    def _():
        msg1_ref[jnp.maximum(j - 1, 0), 128 : 128 + HROWS, :] = z_ref[0:HROWS, :]

    @pl.when(j < 7)
    def _():
        msg1_ref[jnp.minimum(j + 1, 7), 128 : 128 + HROWS, :] = z_ref[64 : 64 + HROWS, :]

    for k in range(PLANES):
        src = b_ref.at[k] if k < K else sh_ref
        edge_ref[k, 0:8, :] = src[0:8, :]
        edge_ref[k, 8:16, :] = src[TR - 8 : TR, :]
    a_ref[...] = jnp.zeros_like(a_ref)
    ln = iota((1, 128), 1)
    for lr in range(6):
        l = 4 * i + lr - 1
        chunk = lattice_chunk(l)
        ok = (ln // 64 == l % 2) & (l >= 0) & (l < 64)
        nd = node_ref[pl.ds(chunk, 1), :]
        a_ref[lr : lr + 1, :] = jnp.where(ok, nd // 2048 - CELL * l, 0).astype(jnp.float32)
        a_ref[8 + lr : 9 + lr, :] = jnp.where(ok, nd % 2048 - CELL * (ln % 64), 0).astype(jnp.float32)
        a_ref[16 + lr : 17 + lr, :] = jnp.where(ok, cond_ref[pl.ds(chunk, 1), :], 0.0)
    wide = dot_nn(a_ref[...], spread(j))
    maps = [extended_rows([wide[8 * n + lr : 8 * n + lr + 1] for lr in range(6)]) for n in range(3)]
    row = iota((ER, EC), 0)
    here = jnp.where(row < TR, row % CELL, jnp.where(row < TR + 4, row - TR, row - TR + 24))
    cols = iota((ER, EC), 1) % CELL
    hit = (maps[0].astype(jnp.int32) == here) & (maps[1].astype(jnp.int32) == cols)
    cm = jnp.where(hit, maps[2], 0.0)
    cm_ref[...] = cm
    tile = cm[0:TR, 0:TC]
    z_scale = jnp.where(tile > 0.0, 1.0 / (4.0 + sh_ref[...] + tile), 0.0)

    def one(k, c):
        down_cells(s_ref, k, b_ref[k] * z_scale)
        return c

    lax.fori_loop(0, K, one, 0)
    v0p = padded(pad_ref, dot_nt(bp_ref[...], m_ref[0]))
    v0p_ref[...] = v0p
    fill(msg0_ref, pack(v0p, gather_bumps(s_ref)))


def columns_kernel(g1_ref, edge_ref, w_ref, up_ref, dn_ref, y_ref, ext_ref):
    _, j = where_am_i()
    y_ref[...] = jnp.zeros_like(y_ref)

    @pl.when(j < 7)
    def _():
        y_ref[0:HROWS, :] = g1_ref[jnp.minimum(j + 1, 7), 128 : 128 + HROWS, :]

    @pl.when(j > 0)
    def _():
        y_ref[64 : 64 + HROWS, :] = g1_ref[jnp.maximum(j - 1, 0), 128 : 128 + HROWS, :]

    yt = y_ref[...].T
    lane = iota((TR, 128), 1)
    for k in range(PLANES):
        right = pltpu.roll(yt, (128 - 3 * k) % 128, 1) if k else yt
        left = pltpu.roll(yt, (61 - 3 * k) % 128, 1) if (61 - 3 * k) % 128 else yt
        w_ref[k] = jnp.where(lane < 3, right, jnp.where(lane >= 125, left, 0.0))
    first = iota((8, EC), 0) < 4
    for k in range(PLANES):
        for side in range(2):
            ext_ref[side, k, :, 0:TC] = edge_ref[k, 8 * side : 8 * side + 8, :]
            ext_ref[side, k, :, TC:EC] = w_ref[k, (TR - 8) * side : (TR - 8) * side + 8, :]
    for p in range(PAIRS):
        q = min(p + PAIRS, PLANES - 1)
        up_ref[p] = jnp.where(first, ext_ref[0, p], pltpu.roll(ext_ref[0, q], 4, 0))
        dn_ref[p] = jnp.where(first, pltpu.roll(ext_ref[1, p], 4, 0), ext_ref[1, q])


def package_all(g_ref, v_ref):
    lane = iota((8, 128), 1) // 32

    def one(c, carry):
        lo = jnp.zeros((8, 128), jnp.float32)
        hi = jnp.zeros((8, 128), jnp.float32)
        for m in range(4):
            x = g_ref[4 * c + m]
            lo = jnp.where(lane == m, pltpu.roll(x, 32 * m, 1) if m else x, lo)
            hi = jnp.where(lane == m, pltpu.roll(x, (32 * m - 32) % 128, 1) if m != 1 else x, hi)
        at = pl.ds(pl.multiple_of(128 * c, 128), 128)
        v_ref[0:8, at] = lo
        v_ref[8:16, at] = hi
        return carry

    lax.fori_loop(0, NB // 128, one, 0, unroll=4)


def own_die(g_ref, i, j):
    lane = iota((8, 128), 1)
    halves = []
    for h in range(2):
        out = jnp.zeros((8, 128), jnp.float32)
        for m in range(4):
            x = g_ref[8 * i + 4 * (j % 2) + m]
            shift = 8 * m - (64 + 32 * h + 8 * (j // 2)) + 128
            x = pltpu.roll(x, shift % 128, 1)
            out = jnp.where((lane >= 8 * m) & (lane < 8 * m + 8), x, out)
        halves.append(out)
    return jnp.concatenate(halves, axis=0)


def own_conductance(cond_ref, i, j):
    q = 8 * i + j
    row = cond_ref[pl.ds(q // 4, 1), :]
    return pltpu.roll(row, (128 - 32 * (q % 4)) % 128, 1)


def spread_package(v_ref, e_ref, x_ref, i, j):
    ln = iota((K, 128), 1)
    for lr in range(6):
        l = 4 * i + lr - 1
        at = pl.ds(pl.multiple_of(128 * lattice_chunk(l), 128), 128)
        x_ref[K * lr : K * (lr + 1), :] = jnp.where(ln // 64 == l % 2, v_ref[:, at], 0.0)
    e_ref[...] = dot_nn(x_ref[...], spread(j))


def others(x, e_ref, k, cm, rd):
    beside = pltpu.roll(x, 1, 0) + pltpu.roll(x, ER - 1, 0)
    beside = beside + pltpu.roll(x, 1, 1) + pltpu.roll(x, EC - 1, 1)
    vp = extended_rows([e_ref[pl.ds(K * lr + k, 1), :] for lr in range(6)])
    return (beside + cm * vp) * rd


def add_dot(r_ref, at, x):
    s = jnp.sum(x, axis=0, keepdims=True)
    r_ref[pl.ds(at, 1), :] = s[:, 0:128] + s[:, 128:256]


def package_step(g_ref, pm_ref, cond_ref, vp, v_ref, pad_ref, i, j):
    y = padded(pad_ref, dot_nt(v_ref[...], pm_ref[...]))
    y = y + own_conductance(cond_ref, i, j) * (vp - own_die(g_ref, i, j))
    return jnp.where(iota((K, 128), 1) < OWN, y, 0.0)


def second_kernel(
    b_ref, sh_ref, w_ref, bot_ref, top_ref, cm_ref, g_ref, g1_ref, m_ref, cond_ref, bp_ref, v0p_ref,
    v1_ref, rd_ref, dg_ref, pm_ref, v1p_ref, y1_ref, msg_ref, r_ref,
    grp_ref, xs_ref, v_ref, e_ref, x_ref, s_ref, pad_ref,
):
    i, j = where_am_i()
    first = iota((8, EC), 0) < 4
    for p in range(PAIRS):
        bot, top = bot_ref[p], top_ref[p]
        grp_ref[p] = jnp.where(first, bot, pltpu.roll(top, 4, 0))
        if p + PAIRS < PLANES:
            grp_ref[p + PAIRS] = jnp.where(first, pltpu.roll(bot, 4, 0), top)

    def gather_plane(main, k):
        xs_ref[0:TR, 0:TC] = main
        xs_ref[0:TR, TC:EC] = w_ref[k]
        xs_ref[TR:ER, :] = grp_ref[k]
        return xs_ref[...]

    sh = gather_plane(sh_ref[...], K)
    cm = cm_ref[...]
    rd_ref[...] = jnp.where(sh > 0.0, 1.0 / (4.0 + sh + cm), 0.0)
    dg_ref[...] = 4.0 + sh[0:TR, 0:TC] + cm[0:TR, 0:TC]
    for d in range(8):
        for t in range(4):
            c = 4 * d + t
            pm_ref[:, 128 * c : 128 * (c + 1)] = g1_ref[d, 32 * t : 32 * (t + 1), :]
    package_all(g_ref, v_ref)
    spread_package(v_ref, e_ref, x_ref, i, j)

    def one(k, c):
        rd = rd_ref[...]
        x0 = gather_plane(b_ref[k], k) * rd
        x1 = x0 - others(x0, e_ref, k, cm_ref[...], rd)
        v1_ref[k] = x1
        dg = dg_ref[...]
        a, b = x0[0:TR, 0:TC], x1[0:TR, 0:TC]
        add_dot(r_ref, k, dg * a * a)
        add_dot(r_ref, K + k, dg * a * b)
        add_dot(r_ref, 2 * K + k, dg * b * b)
        down_cells(s_ref, k, jnp.where(cm_ref[0:TR, 0:TC] > 0.0, b, 0.0))
        return c

    lax.fori_loop(0, K, one, 0)
    v0p = v0p_ref[...]
    bp = padded(pad_ref, bp_ref[...])
    y = package_step(g_ref, pm_ref, cond_ref, v0p, v_ref, pad_ref, i, j)
    v1p = padded(pad_ref, dot_nt(y[:, 0:OWN], m_ref[0]))
    v1p_ref[...] = v1p
    y1_ref[...] = y
    r_ref[0:K, :] += v0p * bp
    r_ref[K : 2 * K, :] += v0p * y
    r_ref[2 * K : 3 * K, :] += v1p * y
    fill(msg_ref, pack(v1p, gather_bumps(s_ref)))


def third_kernel(
    v1_ref, rd_ref, dg_ref, cm_ref, g_ref, pm_ref, m_ref, cond_ref, v1p_ref, y1_ref,
    w_ref, wp_ref, msg_ref, r_ref,
    v_ref, e_ref, x_ref, s_ref, pad_ref,
):
    i, j = where_am_i()
    package_all(g_ref, v_ref)
    spread_package(v_ref, e_ref, x_ref, i, j)

    def one(k, c):
        x1 = v1_ref[k]
        x2 = -others(x1, e_ref, k, cm_ref[...], rd_ref[...])
        w_ref[k] = x2
        dg = dg_ref[...]
        a, b = x1[0:TR, 0:TC], x2[0:TR, 0:TC]
        add_dot(r_ref, k, dg * a * b)
        add_dot(r_ref, K + k, dg * b * b)
        down_cells(s_ref, k, jnp.where(cm_ref[0:TR, 0:TC] > 0.0, b, 0.0))
        return c

    lax.fori_loop(0, K, one, 0)
    v1p = v1p_ref[...]
    y = package_step(g_ref, pm_ref, cond_ref, v1p, v_ref, pad_ref, i, j)
    wp = padded(pad_ref, dot_nt(y[:, 0:OWN], m_ref[0])) - v1p
    wp_ref[...] = wp
    r_ref[0:K, :] += wp * y1_ref[...]
    r_ref[K : 2 * K, :] += wp * (y - y1_ref[...])
    fill(msg_ref, pack(wp, gather_bumps(s_ref)))


def fourth_kernel(
    v2_ref, rd_ref, dg_ref, cm_ref, g_ref, pm_ref, cond_ref, v2p_ref, ra_ref, rb_ref,
    msg_ref,
    v_ref, e_ref, x_ref, pad_ref, r_ref,
):
    i, j = where_am_i()
    package_all(g_ref, v_ref)
    spread_package(v_ref, e_ref, x_ref, i, j)
    r_ref[...] = jnp.zeros_like(r_ref)
    r_ref[0 : 3 * K, :] = ra_ref[...]
    r_ref[3 * K : 5 * K, :] = rb_ref[...]

    def one(k, c):
        x2 = v2_ref[k]
        x3 = x2 - others(x2, e_ref, k, cm_ref[...], rd_ref[...])
        add_dot(r_ref, 5 * K + k, dg_ref[...] * x2[0:TR, 0:TC] * x3[0:TR, 0:TC])
        return c

    lax.fori_loop(0, K, one, 0)
    v2p = v2p_ref[...]
    y = package_step(g_ref, pm_ref, cond_ref, v2p, v_ref, pad_ref, i, j)
    r_ref[5 * K : 6 * K, :] += v2p * y
    sums = dot_nt(jnp.ones((8, 128), jnp.float32), r_ref[...])
    fill(msg_ref, sums[0:1])


def last_kernel(
    g_ref, b_ref, rd_ref, v1_ref, v2_ref, v0p_ref, v1p_ref, v2p_ref,
    xd_ref, xp_ref, c_ref,
):
    total = jnp.sum(g_ref[...], axis=0)
    total = jnp.broadcast_to(total, (8, 128))
    m = [pltpu.roll(total, (128 - K * n) % 128, 1) if n else total for n in range(6)]
    g00, g01, g02, g11, g12, g22 = m[1], m[2], m[3], m[2] + m[3], m[3] + m[4], m[5]
    f1, f2 = g01 / g00, g02 / g00
    a11, a12, h1 = g11 - f1 * g01, g12 - f1 * g02, g00 - f1 * m[0]
    a22, h2 = g22 - f2 * g02, g01 - g00 - f2 * m[0]
    f3 = a12 / a11
    c2 = (h2 - f3 * h1) / (a22 - f3 * a12)
    c1 = (h1 - a12 * c2) / a11
    c0 = (m[0] - g01 * c1 - g02 * c2) / g00
    rd = rd_ref[...]
    at = iota((K, 128), 0) == iota((K, 128), 1)
    cols = []
    for n, c in enumerate((c0, c1, c2)):
        col = jnp.sum(jnp.where(at, c[0:1], 0.0), axis=1, keepdims=True)
        cols.append(col)
        c_ref[n] = jnp.broadcast_to(col, (K, TC))
    xp = cols[0] * v0p_ref[...] + cols[1] * v1p_ref[...] + cols[2] * v2p_ref[...]
    xp_ref[...] = xp[:, 0:OWN]

    def one(k, carry):
        c0, c1, c2 = (c_ref[n, pl.ds(k, 1), :] for n in range(3))
        xd_ref[k] = (c0 * b_ref[k]) * rd + c1 * v1_ref[k] + c2 * v2_ref[k]
        return carry

    lax.fori_loop(0, K, one, 0)


def f32(*shape):
    return jax.ShapeDtypeStruct(shape, jnp.float32)


def vm(*shape):
    return pltpu.VMEM(shape, jnp.float32)


def call(kernel, outs, scratch, args, limit=30, **kw):
    return pl.pallas_call(
        kernel,
        out_shape=outs,
        scratch_shapes=scratch,
        compiler_params=pltpu.CompilerParams(vmem_limit_bytes=limit << 20),
        name=kernel.__name__,
        **kw,
    )(*args)


def swapped(x, axes):
    return lax.all_to_all(x, axes, 0, 0, tiled=True)


def body(
    die_current, die_shunt, pkg_current, pkg_matrix, pkg_block_inv, bump_node, bump_conductance
):
    nodes = bump_node.reshape(NB // 128, 128)
    cond = bump_conductance.reshape(NB // 128, 128)
    stage = [vm(K, NB), vm(6 * K, EC), vm(6 * K, 128), vm(K, 4 * TC), vm(K, 128)]
    gathered = f32(128, 8, 128)
    msg1, msg0, cm, edge, v0p = call(
        first_kernel,
        (f32(8, 128 + HROWS, 128), gathered, f32(ER, EC), f32(PLANES, 16, TC), f32(K, 128)),
        [vm(24, 128), vm(K, 4 * TC), vm(K, 128), vm(128, 128)],
        (die_current, die_shunt, pkg_current, pkg_matrix, pkg_block_inv, nodes, cond),
    )
    g1 = swapped(msg1, COL)
    w, up, dn = call(
        columns_kernel,
        (f32(PLANES, TR, 128), f32(PAIRS, 8, EC), f32(PAIRS, 8, EC)),
        [vm(128, 128), vm(2, PLANES, 8, EC)],
        (g1, edge),
    )
    n = lax.axis_size(ROW)
    bot = lax.ppermute(up, ROW, [(r + 1, r) for r in range(n - 1)])
    top = lax.ppermute(dn, ROW, [(r, r + 1) for r in range(n - 1)])
    g0 = swapped(msg0, ROW_COL)
    v1, rd, dg, pm, v1p, y1, msg, ra = call(
        second_kernel,
        (f32(K, ER, EC), f32(ER, EC), f32(TR, TC), f32(OWN, NB), f32(K, 128), f32(K, 128), gathered, f32(3 * K, 128)),
        [vm(PLANES + 1, 8, EC), vm(ER, EC)] + stage,
        (die_current, die_shunt, w, bot, top, cm, g0, g1, pkg_block_inv, cond, pkg_current, v0p),
    )
    g = swapped(msg, ROW_COL)
    v2, v2p, msg, rb = call(
        third_kernel,
        (f32(K, ER, EC), f32(K, 128), gathered, f32(2 * K, 128)),
        stage,
        (v1, rd, dg, cm, g, pm, pkg_block_inv, cond, v1p, y1),
    )
    g = swapped(msg, ROW_COL)
    msg = call(
        fourth_kernel,
        f32(128, 1, 128),
        stage[:3] + [vm(K, 128), vm(128, 128)],
        (v2, rd, dg, cm, g, pm, cond, v2p, ra, rb),
    )
    g = swapped(msg, ROW_COL)
    whole = lambda *s: pl.BlockSpec(s, lambda t: (0,) * len(s))
    return call(
        last_kernel,
        (f32(K, TR, TC), f32(K, OWN)),
        [vm(3, K, TC)],
        (g, die_current, rd, v1, v2, v0p, v1p, v2p),
        grid=(1,),
        in_specs=[
            whole(128, 1, 128), whole(K, TR, TC), whole(TR, TC), whole(K, TR, TC), whole(K, TR, TC),
            whole(K, 128), whole(K, 128), whole(K, 128),
        ],
        out_specs=(whole(K, TR, TC), whole(K, OWN)),
    )


def solution(mesh):
    torus = Mesh(mesh.devices.reshape(2, 4, 2, 4, 2), ROW_COL)
    placed = (
        P(None, ROW, COL),
        P(ROW, COL),
        P(None, ROW_COL),
        P(ROW, COL),
        P(ROW_COL, None, None),
        P(),
        P(),
    )
    return jax.shard_map(
        body,
        mesh=torus,
        in_specs=placed,
        out_specs=(P(None, ROW, COL), P(None, ROW_COL)),
        check_vma=False,
    )
```

```python
import functools

import jax
import jax.numpy as jnp
from jax import lax
from jax.experimental import pallas as pl
from jax.experimental.pallas import tpu as pltpu
from jax.sharding import Mesh
from jax.sharding import PartitionSpec as P

ROW = ("row_0", "row_1", "row_2")
COL = ("col_0", "col_1")
ROW_COL = ("row_0", "row_1", "row_2", "col_0", "col_1")

K = 16
TR, TC = 128, 256
ER, EC = 136, 384
CELL = 32
PLANES = K + 1
PAIRS = 9
HROWS = 56
OWN = 32
NB = 4096
HI = lax.Precision.HIGHEST


def iota(shape, dim):
    return lax.broadcasted_iota(jnp.int32, shape, dim)


def where_am_i():
    i = (lax.axis_index("row_0") * 4 + lax.axis_index("row_1")) * 2 + lax.axis_index("row_2")
    j = lax.axis_index("col_0") * 2 + lax.axis_index("col_1")
    return i, j


def dot_nt(a, b):
    return lax.dot_general(
        a, b, (((1,), (1,)), ((), ())), precision=HI, preferred_element_type=jnp.float32
    )


def dot_nn(a, b):
    return jnp.dot(a, b, precision=HI, preferred_element_type=jnp.float32)


def spread(j):
    group = iota((128, EC), 1) // CELL
    cell = jnp.where(group <= 8, 8 * j + group, jnp.where(group == 11, 8 * j - 1, -5))
    return (iota((128, EC), 0) % 64 == cell).astype(jnp.float32)


def lattice_chunk(l):
    return jnp.clip(l // 2, 0, NB // 128 - 1)


def extended_rows(parts):
    body = [jnp.broadcast_to(p, (CELL, EC)) for p in parts[1:5]]
    edge = jnp.where(iota((8, EC), 0) < 4, parts[5], parts[0])
    return jnp.concatenate(body + [edge], axis=0)


def padded(scr, x):
    scr[...] = jnp.zeros_like(scr)
    scr[:, 0 : x.shape[1]] = x
    return scr[...]


def pack(vp, vd):
    lane = iota((8, 128), 1)
    hi = pltpu.roll(vp[8:16], 32, 1)
    out = jnp.where(lane < 32, vp[0:8], hi)
    out = jnp.where(lane < 64, out, pltpu.roll(vd[0:8], 64, 1))
    return jnp.where(lane < 96, out, pltpu.roll(vd[8:16], 96, 1))


def gather_bumps(s_ref):
    at = iota((4 * TC, 128), 0)
    pick = (at // TC * 8 + at % TC // CELL == iota((4 * TC, 128), 1)).astype(jnp.float32)
    return dot_nn(s_ref[...], pick)


def down_cells(s_ref, k, z):
    for lr in range(4):
        rows = z[CELL * lr : CELL * (lr + 1)]
        s_ref[pl.ds(k, 1), TC * lr : TC * (lr + 1)] = jnp.sum(rows, axis=0, keepdims=True)


SENDS = 8


def send(msg_hbm, pay_ref, sems, pay):
    n = pay_ref.shape[0]
    for d in range(n):
        pay_ref[d] = pay
    copies = [
        pltpu.make_async_copy(pay_ref, msg_hbm.at[n * c : n * (c + 1)], sems.at[c]) for c in range(SENDS)
    ]
    for c in copies:
        c.start()
    for c in copies:
        c.wait()


def load_kernel(mv, b_ref, sh_ref, p_ref, msg_hbm, edge_ref, z_ref, sems):
    _, j = where_am_i()
    lane = iota((TR, 128), 1)
    z = jnp.zeros((TR, 128), jnp.float32)
    mv.wait(1)
    for k in [K] + list(range(K)):
        if k < K and k % 4 == 0:
            mv.wait(0, k // 4)
        src = b_ref.at[k] if k < K else sh_ref
        lo = pltpu.roll(src[:, 0:128], 3 * k, 1) if k else src[:, 0:128]
        up = pltpu.roll(src[:, 128:256], (64 + 3 * k - 125) % 128, 1)
        z = jnp.where((lane >= 3 * k) & (lane < 3 * k + 3), lo, z)
        z = jnp.where((lane >= 64 + 3 * k) & (lane < 67 + 3 * k), up, z)
        edge_ref[k, 0:8, :] = src[0:8, :]
        edge_ref[k, 8:16, :] = src[TR - 8 : TR, :]
    mv.flush(1)
    mv.wait(2)
    rows = [
        pltpu.make_async_copy(
            p_ref.at[:, :, 128 * t : 128 * (t + 1)],
            msg_hbm.at[:, 32 * t : 32 * (t + 1), :],
            sems.at[t],
        )
        for t in range(4)
    ]
    for c in rows:
        c.start()
    z_ref[...] = z.T
    side = lambda at, to, n: pltpu.make_async_copy(
        z_ref.at[at : at + HROWS, :], msg_hbm.at[to, 128 : 128 + HROWS, :], sems.at[n]
    )
    sides = [side(0, jnp.maximum(j - 1, 0), 4), side(64, jnp.minimum(j + 1, 7), 5)]
    for c in sides:
        c.start()
    for c in sides + rows:
        c.wait()


def start_kernel(
    mv, b_ref, sh_ref, bp_ref, m_ref, node_ref, cond_ref,
    msg_hbm, cm_ref, v0p_ref,
    a_ref, s_ref, pad_ref, pay_ref, sems,
):
    i, j = where_am_i()
    for n in (4, 5):
        mv.wait(n)
    a_ref[...] = jnp.zeros_like(a_ref)
    ln = iota((1, 128), 1)
    for lr in range(6):
        l = 4 * i + lr - 1
        chunk = lattice_chunk(l)
        ok = (ln // 64 == l % 2) & (l >= 0) & (l < 64)
        nd = node_ref[pl.ds(chunk, 1), :]
        a_ref[lr : lr + 1, :] = jnp.where(ok, nd // 2048 - CELL * l, 0).astype(jnp.float32)
        a_ref[8 + lr : 9 + lr, :] = jnp.where(ok, nd % 2048 - CELL * (ln % 64), 0).astype(jnp.float32)
        a_ref[16 + lr : 17 + lr, :] = jnp.where(ok, cond_ref[pl.ds(chunk, 1), :], 0.0)
    wide = dot_nn(a_ref[...], spread(j))
    maps = [extended_rows([wide[8 * n + lr : 8 * n + lr + 1] for lr in range(6)]) for n in range(3)]
    row = iota((ER, EC), 0)
    here = jnp.where(row < TR, row % CELL, jnp.where(row < TR + 4, row - TR, row - TR + 24))
    cols = iota((ER, EC), 1) % CELL
    hit = (maps[0].astype(jnp.int32) == here) & (maps[1].astype(jnp.int32) == cols)
    cm = jnp.where(hit, maps[2], 0.0)
    cm_ref[...] = cm
    mv.flush(1)
    mv.wait(1)
    here = cm[0:TR, 0:TC]
    z_scale = jnp.where(here > 0.0, 1.0 / (4.0 + sh_ref[...] + here), 0.0)

    def one(k, c):
        down_cells(s_ref, k, b_ref[k] * z_scale)
        return c

    mv.wait(0)
    lax.fori_loop(0, K, one, 0)
    mv.wait(2)
    mv.wait(3)
    v0p = padded(pad_ref, dot_nt(bp_ref[...], m_ref[0]))
    v0p_ref[...] = v0p
    mv.flush(2)
    send(msg_hbm, pay_ref, sems, pack(v0p, gather_bumps(s_ref)))


def columns_kernel(mv, g1_ref, edge_ref, w_ref, up_ref, dn_ref, y_ref, ext_ref):
    _, j = where_am_i()
    y_ref[...] = jnp.zeros_like(y_ref)

    @pl.when(j < 7)
    def _():
        y_ref[0:HROWS, :] = g1_ref[jnp.minimum(j + 1, 7), 128 : 128 + HROWS, :]

    @pl.when(j > 0)
    def _():
        y_ref[64 : 64 + HROWS, :] = g1_ref[jnp.maximum(j - 1, 0), 128 : 128 + HROWS, :]

    yt = y_ref[...].T
    lane = iota((TR, 128), 1)
    for k in range(PLANES):
        right = pltpu.roll(yt, (128 - 3 * k) % 128, 1) if k else yt
        left = pltpu.roll(yt, (61 - 3 * k) % 128, 1) if (61 - 3 * k) % 128 else yt
        w_ref[k] = jnp.where(lane < 3, right, jnp.where(lane >= 125, left, 0.0))
    first = iota((8, EC), 0) < 4
    mv.wait(1)
    for k in range(PLANES):
        for side in range(2):
            ext_ref[side, k, :, 0:TC] = edge_ref[k, 8 * side : 8 * side + 8, :]
            ext_ref[side, k, :, TC:EC] = w_ref[k, (TR - 8) * side : (TR - 8) * side + 8, :]
    for p in range(PAIRS):
        q = min(p + PAIRS, PLANES - 1)
        up_ref[p] = jnp.where(first, ext_ref[0, p], pltpu.roll(ext_ref[0, q], 4, 0))
        dn_ref[p] = jnp.where(first, pltpu.roll(ext_ref[1, p], 4, 0), ext_ref[1, q])
    mv.flush(0)


def whole_plane(xs_ref, main, w_ref, grp_ref, k):
    xs_ref[0:TR, 0:TC] = main
    xs_ref[0:TR, TC:EC] = w_ref[k]
    xs_ref[TR:ER, :] = grp_ref[k]
    return xs_ref[...]


def package_all(g_ref, v_ref):
    lane = iota((8, 128), 1) // 32

    def one(c, carry):
        lo = jnp.zeros((8, 128), jnp.float32)
        hi = jnp.zeros((8, 128), jnp.float32)
        for m in range(4):
            x = g_ref[4 * c + m]
            lo = jnp.where(lane == m, pltpu.roll(x, 32 * m, 1) if m else x, lo)
            hi = jnp.where(lane == m, pltpu.roll(x, (32 * m - 32) % 128, 1) if m != 1 else x, hi)
        at = pl.ds(pl.multiple_of(128 * c, 128), 128)
        v_ref[0:8, at] = lo
        v_ref[8:16, at] = hi
        return carry

    lax.fori_loop(0, NB // 128, one, 0, unroll=4)


def own_die(g_ref, i, j):
    lane = iota((8, 128), 1)
    halves = []
    for h in range(2):
        out = jnp.zeros((8, 128), jnp.float32)
        for m in range(4):
            x = g_ref[8 * i + 4 * (j % 2) + m]
            shift = 8 * m - (64 + 32 * h + 8 * (j // 2)) + 128
            x = pltpu.roll(x, shift % 128, 1)
            out = jnp.where((lane >= 8 * m) & (lane < 8 * m + 8), x, out)
        halves.append(out)
    return jnp.concatenate(halves, axis=0)


def own_conductance(cond_ref, i, j):
    q = 8 * i + j
    row = cond_ref[pl.ds(q // 4, 1), :]
    return pltpu.roll(row, (128 - 32 * (q % 4)) % 128, 1)


def around(v_ref, x_ref, i):
    ln = iota((K, 128), 1)
    for lr in range(6):
        l = 4 * i + lr - 1
        at = pl.ds(pl.multiple_of(128 * lattice_chunk(l), 128), 128)
        x_ref[K * lr : K * (lr + 1), :] = jnp.where(ln // 64 == l % 2, v_ref[:, at], 0.0)


def coupled(e_ref, k):
    return extended_rows([e_ref[pl.ds(K * lr + k, 1), :] for lr in range(6)])


def beside(x):
    out = pltpu.roll(x, 1, 0) + pltpu.roll(x, ER - 1, 0)
    return out + pltpu.roll(x, 1, 1) + pltpu.roll(x, EC - 1, 1)


def add_dot(r_ref, at, x):
    s = jnp.sum(x, axis=0, keepdims=True)
    r_ref[pl.ds(at, 1), :] = s[:, 0:128] + s[:, 128:256]


def tile(x):
    return x[0:TR, 0:TC]


def prepare_kernel(
    mv, b_ref, sh_ref, w_ref, bot_ref, top_ref, cm_ref, g1_ref,
    grp_ref, bump_ref, rd_ref, dg_ref, cr_ref, pm_ref,
    xs_ref, s_ref,
):
    for d in range(8):
        for t in range(4):
            c = 4 * d + t
            pm_ref[:, 128 * c : 128 * (c + 1)] = g1_ref[d, 32 * t : 32 * (t + 1), :]
    mv.flush(5)
    mv.wait(1)
    mv.wait(5)
    first = iota((8, EC), 0) < 4
    for p in range(PAIRS):
        bot, top = bot_ref[p], top_ref[p]
        grp_ref[p] = jnp.where(first, bot, pltpu.roll(top, 4, 0))
        if p + PAIRS < PLANES:
            grp_ref[p + PAIRS] = jnp.where(first, pltpu.roll(bot, 4, 0), top)
    mv.flush(0)
    mv.wait(2)
    sh = whole_plane(xs_ref, sh_ref[...], w_ref, grp_ref, K)
    cm = cm_ref[...]
    rd = jnp.where(sh > 0.0, 1.0 / (4.0 + sh + cm), 0.0)
    rd_ref[...] = rd
    cr_ref[...] = cm * rd
    dg_ref[...] = 4.0 + tile(sh) + tile(cm)
    for n in (2, 3, 4):
        mv.flush(n)

    def one(k, c):
        rd = rd_ref[...]
        x0 = whole_plane(xs_ref, b_ref[k], w_ref, grp_ref, k) * rd
        pre = x0 - beside(x0) * rd
        down_cells(s_ref, k, jnp.where(tile(cm_ref) > 0.0, tile(pre), 0.0))
        return c

    for c in range(CHUNKS):
        mv.wait(0, c)
        lax.fori_loop(4 * c, 4 * c + 4, one, 0)
    s_ref[K : K + 8, :] = jnp.zeros((8, 4 * TC), jnp.float32)
    down_cells(s_ref, K, tile(cm_ref))
    down_cells(s_ref, K + 1, tile(cr_ref))
    bump_ref[...] = gather_bumps(s_ref)
    mv.flush(1)


def package_kernel(
    step, mv, g_ref, pm_ref, m_ref, cond_ref, bump_ref, const_ref, vp_ref,
    out_ref, vd_ref, y_ref, x_ref, msg_hbm,
    v_ref, pad_ref, pay_ref, sems,
):
    i, j = where_am_i()
    package_all(g_ref, v_ref)
    for n in range(1, 7):
        if n in mv.ins:
            mv.wait(n)
    vp = vp_ref[...]
    y = padded(pad_ref, dot_nt(v_ref[...], pm_ref[...]))
    y = y + own_conductance(cond_ref, i, j) * (vp - own_die(g_ref, i, j))
    y = jnp.where(iota((K, 128), 1) < OWN, y, 0.0)
    out = padded(pad_ref, dot_nt(y[:, 0:OWN], m_ref[0]))
    if step == 2:
        out = out - vp
    vd = bump_ref[0:K, :] - const_ref[K + 1 : K + 2, :] * at_tile(v_ref, i, j)
    y_ref[...] = y
    out_ref[...] = out
    vd_ref[...] = vd
    around(v_ref, x_ref, i)
    for n in range(4):
        mv.flush(n)
    send(msg_hbm, pay_ref, sems, pack(out, vd))


def at_tile(v_ref, i, j):
    ln = iota((K, 128), 1)
    out = jnp.zeros((K, 128), jnp.float32)
    for lr in range(4):
        l = 4 * i + lr
        at = pl.ds(pl.multiple_of(128 * lattice_chunk(l), 128), 128)
        x = pltpu.roll(v_ref[:, at], (8 * lr - 64 * (l % 2) - 8 * j + 256) % 128, 1)
        out = jnp.where((ln >= 8 * lr) & (ln < 8 * lr + 8), x, out)
    return out


def second_kernel(
    mv, b_ref, w_ref, grp_ref, rd_ref, dg_ref, cr_ref, x_ref, bp_ref, v0p_ref, v1p_ref, y1_ref,
    v1_ref, bump_ref, r_ref,
    e_ref, s_ref, pad_ref, xs_ref,
):
    i, j = where_am_i()
    for n in range(1, 11):
        mv.wait(n)
    e_ref[...] = dot_nn(x_ref[...], spread(j))

    def one(k, c):
        rd, dg = rd_ref[...], dg_ref[...]
        x0 = whole_plane(xs_ref, b_ref[k], w_ref, grp_ref, k) * rd
        x1 = x0 - (beside(x0) * rd + cr_ref[...] * coupled(e_ref, k))
        v1_ref[k] = x1
        down_cells(s_ref, k, jnp.where(tile(cr_ref) > 0.0, tile(-beside(x1) * rd), 0.0))
        a, b = tile(x0), tile(x1)
        add_dot(r_ref, k, dg * a * a)
        add_dot(r_ref, K + k, dg * a * b)
        add_dot(r_ref, 2 * K + k, dg * b * b)
        return c

    for c in range(CHUNKS):
        mv.wait(0, c)
        lax.fori_loop(4 * c, 4 * c + 4, one, 0)
        mv.flush(0, c)
    bump_ref[...] = gather_bumps(s_ref)
    v0p, v1p, y1 = v0p_ref[...], v1p_ref[...], y1_ref[...]
    bp = padded(pad_ref, bp_ref[...])
    r_ref[0:K, :] += v0p * bp
    r_ref[K : 2 * K, :] += v0p * y1
    r_ref[2 * K : 3 * K, :] += v1p * y1
    mv.flush(2)


def third_kernel(
    mv, v1_ref, rd_ref, dg_ref, cr_ref, x_ref, wp_ref, y1_ref, y2_ref, ra_ref,
    wt_ref, r_ref,
    e_ref,
):
    i, j = where_am_i()
    for n in range(1, 9):
        mv.wait(n)
    e_ref[...] = dot_nn(x_ref[...], spread(j))
    r_ref[6 * K :, :] = jnp.zeros((2 * K, 128), jnp.float32)
    r_ref[0 : 3 * K, :] = ra_ref[...]

    def one(k, c):
        dg = dg_ref[...]
        x1 = v1_ref[k]
        w = -(beside(x1) * rd_ref[...] + cr_ref[...] * coupled(e_ref, k))
        a, b = tile(x1), tile(w)
        wt_ref[k] = b
        add_dot(r_ref, 3 * K + k, dg * a * b)
        add_dot(r_ref, 4 * K + k, dg * b * b)
        add_dot(r_ref, 5 * K + k, dg * b * (b - tile(beside(w)) * tile(rd_ref)))
        return c

    for c in range(CHUNKS):
        mv.wait(0, c)
        lax.fori_loop(4 * c, 4 * c + 4, one, 0)
        mv.flush(0, c)
    wp, y1, y2 = wp_ref[...], y1_ref[...], y2_ref[...]
    r_ref[3 * K : 4 * K, :] += wp * y1
    r_ref[4 * K : 5 * K, :] += wp * (y2 - y1)


def fourth_kernel(
    mv, g_ref, pm_ref, cond_ref, const_ref, wp_ref, wd_ref, ra_ref,
    msg_ref,
    v_ref, pad_ref, r_ref,
):
    i, j = where_am_i()
    package_all(g_ref, v_ref)
    for n in range(1, 6):
        mv.wait(n)
    wp = wp_ref[...]
    y = padded(pad_ref, dot_nt(v_ref[...], pm_ref[...]))
    y = y + own_conductance(cond_ref, i, j) * (wp - own_die(g_ref, i, j))
    y = jnp.where(iota((K, 128), 1) < OWN, y, 0.0)
    r_ref[...] = ra_ref[...]
    r_ref[5 * K : 6 * K, :] += wp * y - const_ref[K : K + 1, :] * wd_ref[...] * at_tile(v_ref, i, j)
    sums = dot_nt(jnp.ones((8, 128), jnp.float32), r_ref[...])

    def one(d, c):
        msg_ref[d] = sums[0:1]
        return c

    lax.fori_loop(0, msg_ref.shape[0], one, 0, unroll=8)


def last_kernel(
    mv, g_ref, b_ref, rd_ref, v1_ref, v2_ref, v0p_ref, v1p_ref, v2p_ref,
    xd_ref, xp_ref, c_ref,
):
    total = jnp.sum(g_ref[...], axis=0)
    total = jnp.broadcast_to(total, (8, 128))
    m = [pltpu.roll(total, (128 - K * n) % 128, 1) if n else total for n in range(6)]
    g00, g01, g02, g11, g12, g22 = m[1], m[2], m[3], m[2] + m[3], m[3] + m[4], m[5]
    f1, f2 = g01 / g00, g02 / g00
    a11, a12, h1 = g11 - f1 * g01, g12 - f1 * g02, g00 - f1 * m[0]
    a22, h2 = g22 - f2 * g02, g01 - g00 - f2 * m[0]
    f3 = a12 / a11
    c2 = (h2 - f3 * h1) / (a22 - f3 * a12)
    c1 = (h1 - a12 * c2) / a11
    c0 = (m[0] - g01 * c1 - g02 * c2) / g00
    rd = tile(rd_ref)
    at = iota((K, 128), 0) == iota((K, 128), 1)
    cols = []
    for n, c in enumerate((c0, c1, c2)):
        col = jnp.sum(jnp.where(at, c[0:1], 0.0), axis=1, keepdims=True)
        cols.append(col)
        c_ref[n] = jnp.broadcast_to(col, (K, TC))
    xp = cols[0] * v0p_ref[...] + cols[1] * v1p_ref[...] + cols[2] * v2p_ref[...]
    xp_ref[...] = xp[:, 0:OWN]

    def one(k, carry):
        c0, c1, c2 = (c_ref[n, pl.ds(k, 1), :] for n in range(3))
        xd_ref[k] = (c0 * b_ref[k]) * rd + c1 * tile(v1_ref.at[k]) + c2 * v2_ref[k]
        return carry

    lax.fori_loop(0, K, one, 0)


def f32(*shape):
    return jax.ShapeDtypeStruct(shape, jnp.float32)


def vm(*shape):
    return pltpu.VMEM(shape, jnp.float32)


CHUNKS = 4


class Moves:
    def __init__(self):
        self.ins, self.outs, self.pending = {}, {}, []

    def wait(self, n, chunk=None):
        for c in [chunk] if chunk is not None else range(len(self.ins[n])):
            self.ins[n][c].wait()
            self.ins[n][c] = None

    def flush(self, n, chunk=None):
        for c in [chunk] if chunk is not None else range(len(self.outs[n])):
            self.outs[n][c].start()
            self.pending.append(self.outs[n][c])


def parts(ref, mode):
    if mode == "h":
        return [ref]
    step = ref.shape[0] // CHUNKS
    return [ref.at[step * c : step * (c + 1)] for c in range(CHUNKS)]


def call(kernel, ins, outs, scratch, limit=14, **kw):
    imode, omode = [m for _, m in ins], [m for _, m in outs]
    moved = [jax.ShapeDtypeStruct(x.shape, x.dtype) for x, m in ins + outs if m in "hc"]
    count = sum({"h": 1, "c": CHUNKS}.get(m, 0) for m in imode + omode)

    def wrapped(*refs):
        ni, no, nm = len(ins), len(outs), len(moved)
        hbm, bufs, sems, own = refs[: ni + no], list(refs[ni + no :][:nm]), refs[ni + no + nm], refs[ni + no + nm + 1 :]
        mv, given, sem = Moves(), [], 0
        for n, (ref, mode) in enumerate(zip(hbm, imode + omode)):
            if mode not in "hc":
                given.append(ref)
                continue
            buf = bufs.pop(0)
            given.append(buf)
            copies = []
            for x, y in zip(parts(ref, mode), parts(buf, mode)):
                x, y = (x, y) if n < ni else (y, x)
                copies.append(pltpu.make_async_copy(x, y, sems.at[sem]))
                sem += 1
            (mv.ins if n < ni else mv.outs)[n if n < ni else n - ni] = copies
        for copies in sorted(mv.ins.values(), key=len):
            for c in copies:
                c.start()
        kernel(mv, *given, *own)
        for copies in mv.ins.values():
            assert all(c is None for c in copies)
        for c in mv.pending:
            c.wait()

    space = lambda m: pl.BlockSpec(memory_space=pltpu.VMEM if m == "v" else pltpu.HBM)
    return pl.pallas_call(
        wrapped,
        out_shape=tuple(x if m == "v" else pltpu.HBM(x.shape, x.dtype) for x, m in outs),
        in_specs=[space(m) for m in imode],
        out_specs=tuple(space(m) for m in omode),
        scratch_shapes=[pltpu.VMEM(x.shape, x.dtype) for x in moved]
        + [pltpu.SemaphoreType.DMA((max(count, 1),))] + scratch,
        compiler_params=pltpu.CompilerParams(vmem_limit_bytes=limit << 20),
        name=getattr(kernel, "func", kernel).__name__,
        **kw,
    )(*[x if m == "v" else pltpu.with_memory_space_constraint(x, pltpu.HBM) for x, m in ins])


def swapped(x, axes):
    return lax.all_to_all(x, axes, 0, 0, tiled=True)


def body(
    die_current, die_shunt, pkg_current, pkg_matrix, pkg_block_inv, bump_node, bump_conductance
):
    nodes = bump_node.reshape(NB // 128, 128)
    cond = bump_conductance.reshape(NB // 128, 128)
    b, sh, bp, m = die_current, die_shunt, pkg_current, pkg_block_inv
    gathered, small, ext, die = f32(128, 8, 128), f32(K, 128), f32(K, ER, EC), f32(K, TR, TC)
    lattice = f32(6 * K, 128)
    payload = [vm(128 // SENDS, 8, 128), pltpu.SemaphoreType.DMA((SENDS,))]
    msg1, edge = call(
        load_kernel,
        [(b, "c"), (sh, "h"), (pkg_matrix.reshape(8, OWN, 512), "h")],
        [(f32(8, 128 + HROWS, 128), "r"), (f32(PLANES, 16, TC), "h")],
        [vm(128, 128), pltpu.SemaphoreType.DMA((6,))],
    )
    g1 = swapped(msg1, COL)
    msg, cm, v0p = call(
        start_kernel,
        [(b, "h"), (sh, "h"), (bp, "h"), (m, "h"), (nodes, "h"), (cond, "h")],
        [(gathered, "r"), (f32(ER, EC), "h"), (small, "h")],
        [vm(24, 128), vm(K, 4 * TC), vm(K, 128)] + payload,
    )
    g = swapped(msg, ROW_COL)
    side, up, dn = call(
        columns_kernel,
        [(g1, "v"), (edge, "h")],
        [(f32(PLANES, TR, 128), "h"), (f32(PAIRS, 8, EC), "v"), (f32(PAIRS, 8, EC), "v")],
        [vm(128, 128), vm(2, PLANES, 8, EC)],
    )
    n = lax.axis_size(ROW)
    bot = lax.ppermute(up, ROW, [(r + 1, r) for r in range(n - 1)])
    top = lax.ppermute(dn, ROW, [(r, r + 1) for r in range(n - 1)])
    grp, bump1, rd, dg, cr, pm = call(
        prepare_kernel,
        [(b, "c"), (sh, "h"), (side, "h"), (bot, "v"), (top, "v"), (cm, "h"), (g1, "v")],
        [
            (f32(PLANES, 8, EC), "h"), (f32(K + 8, 128), "h"), (f32(ER, EC), "h"),
            (f32(TR, TC), "h"), (f32(ER, EC), "h"), (f32(OWN, NB), "h"),
        ],
        [vm(ER, EC), vm(K + 8, 4 * TC)],
    )
    step = [vm(K, NB), vm(K, 128)] + payload
    results = [(small, "h"), (small, "h"), (small, "h"), (lattice, "h"), (gathered, "r")]
    v1p, _, y1, near, msg = call(
        functools.partial(package_kernel, 1),
        [(g, "v"), (pm, "h"), (m, "h"), (cond, "h"), (bump1, "h"), (bump1, "h"), (v0p, "h")],
        results,
        step,
    )
    g = swapped(msg, ROW_COL)
    v1, bump2, r = call(
        second_kernel,
        [(b, "c")] + [(x, "h") for x in (side, grp, rd, dg, cr, near, bp, v0p, v1p, y1)],
        [(ext, "c"), (small, "v"), (f32(3 * K, 128), "h")],
        [vm(6 * K, EC), vm(K, 4 * TC), vm(K, 128), vm(ER, EC)],
    )
    wp, wd, y2, near, msg = call(
        functools.partial(package_kernel, 2),
        [(g, "v"), (pm, "h"), (m, "h"), (cond, "h"), (bump2, "v"), (bump1, "h"), (v1p, "h")],
        results,
        step,
    )
    g = swapped(msg, ROW_COL)
    w, r = call(
        third_kernel,
        [(v1, "c")] + [(x, "h") for x in (rd, dg, cr, near, wp, y1, y2, r)],
        [(die, "c"), (f32(128, 128), "v")],
        [vm(6 * K, EC)],
    )
    (msg,) = call(
        fourth_kernel,
        [(g, "v")] + [(x, "h") for x in (pm, cond, bump1, wp, wd)] + [(r, "v")],
        [(f32(128, 1, 128), "v")],
        [vm(K, NB), vm(K, 128), vm(128, 128)],
    )
    g = swapped(msg, ROW_COL)
    return call(
        last_kernel,
        [(x, "v") for x in (g, b, rd, v1, w, v0p, v1p, wp)],
        [(die, "v"), (f32(K, OWN), "v")],
        [vm(3, K, TC)],
    )


def solution(mesh):
    torus = Mesh(mesh.devices.reshape(2, 4, 2, 4, 2), ROW_COL)
    placed = (
        P(None, ROW, COL),
        P(ROW, COL),
        P(None, ROW_COL),
        P(ROW, COL),
        P(ROW_COL, None, None),
        P(),
        P(),
    )
    return jax.shard_map(
        body,
        mesh=torus,
        in_specs=placed,
        out_specs=(P(None, ROW, COL), P(None, ROW_COL)),
        check_vma=False,
    )
```

```python
import functools

import jax
import jax.numpy as jnp
from jax import lax
from jax.experimental import pallas as pl
from jax.experimental.pallas import tpu as pltpu
from jax.sharding import Mesh
from jax.sharding import PartitionSpec as P

ROW = ("row_0", "row_1", "row_2")
COL = ("col_0", "col_1")
ROW_COL = ("row_0", "row_1", "row_2", "col_0", "col_1")

K = 16
TR, TC = 128, 256
ER, EC = 136, 384
CELL = 32
PLANES = K + 1
PAIRS = 9
HROWS = 56
OWN = 32
NB = 4096
HI = lax.Precision.HIGHEST


def iota(shape, dim):
    return lax.broadcasted_iota(jnp.int32, shape, dim)


def where_am_i():
    i = (lax.axis_index("row_0") * 4 + lax.axis_index("row_1")) * 2 + lax.axis_index("row_2")
    j = lax.axis_index("col_0") * 2 + lax.axis_index("col_1")
    return i, j


def dot_nt(a, b):
    return lax.dot_general(
        a, b, (((1,), (1,)), ((), ())), precision=HI, preferred_element_type=jnp.float32
    )


def dot_nn(a, b):
    return jnp.dot(a, b, precision=HI, preferred_element_type=jnp.float32)


def spread(j):
    group = iota((128, EC), 1) // CELL
    cell = jnp.where(group <= 8, 8 * j + group, jnp.where(group == 11, 8 * j - 1, -5))
    return (iota((128, EC), 0) % 64 == cell).astype(jnp.float32)


def lattice_chunk(l):
    return jnp.clip(l // 2, 0, NB // 128 - 1)


def extended_rows(parts):
    body = [jnp.broadcast_to(p, (CELL, EC)) for p in parts[1:5]]
    edge = jnp.where(iota((8, EC), 0) < 4, parts[5], parts[0])
    return jnp.concatenate(body + [edge], axis=0)


def padded(scr, x):
    scr[...] = jnp.zeros_like(scr)
    scr[:, 0 : x.shape[1]] = x
    return scr[...]


def pack(vp, vd):
    lane = iota((8, 128), 1)
    hi = pltpu.roll(vp[8:16], 32, 1)
    out = jnp.where(lane < 32, vp[0:8], hi)
    out = jnp.where(lane < 64, out, pltpu.roll(vd[0:8], 64, 1))
    return jnp.where(lane < 96, out, pltpu.roll(vd[8:16], 96, 1))


def gather_bumps(s_ref):
    at = iota((4 * TC, 128), 0)
    pick = (at // TC * 8 + at % TC // CELL == iota((4 * TC, 128), 1)).astype(jnp.float32)
    return dot_nn(s_ref[...], pick)


def down_cells(s_ref, k, z):
    for lr in range(4):
        rows = z[CELL * lr : CELL * (lr + 1)]
        s_ref[pl.ds(k, 1), TC * lr : TC * (lr + 1)] = jnp.sum(rows, axis=0, keepdims=True)


SENDS = 8


def send(msg_hbm, pay_ref, sems, pay):
    n = pay_ref.shape[0]
    for d in range(n):
        pay_ref[d] = pay
    copies = [
        pltpu.make_async_copy(pay_ref, msg_hbm.at[n * c : n * (c + 1)], sems.at[c]) for c in range(SENDS)
    ]
    for c in copies:
        c.start()
    for c in copies:
        c.wait()


def load_kernel(mv, b_ref, sh_ref, p_ref, msg_hbm, edge_ref, z_ref, sems):
    _, j = where_am_i()
    lane = iota((TR, 128), 1)
    z = jnp.zeros((TR, 128), jnp.float32)
    mv.wait(1)
    for k in [K] + list(range(K)):
        if k < K and k % 4 == 0:
            mv.wait(0, k // 4)
        src = b_ref.at[k] if k < K else sh_ref
        lo = pltpu.roll(src[:, 0:128], 3 * k, 1) if k else src[:, 0:128]
        up = pltpu.roll(src[:, 128:256], (64 + 3 * k - 125) % 128, 1)
        z = jnp.where((lane >= 3 * k) & (lane < 3 * k + 3), lo, z)
        z = jnp.where((lane >= 64 + 3 * k) & (lane < 67 + 3 * k), up, z)
        edge_ref[k, 0:8, :] = src[0:8, :]
        edge_ref[k, 8:16, :] = src[TR - 8 : TR, :]
    mv.flush(1)
    mv.wait(2)
    rows = [
        pltpu.make_async_copy(
            p_ref.at[:, :, 128 * t : 128 * (t + 1)],
            msg_hbm.at[:, 32 * t : 32 * (t + 1), :],
            sems.at[t],
        )
        for t in range(4)
    ]
    for c in rows:
        c.start()
    z_ref[...] = z.T
    side = lambda at, to, n: pltpu.make_async_copy(
        z_ref.at[at : at + HROWS, :], msg_hbm.at[to, 128 : 128 + HROWS, :], sems.at[n]
    )
    sides = [side(0, jnp.maximum(j - 1, 0), 4), side(64, jnp.minimum(j + 1, 7), 5)]
    for c in sides:
        c.start()
    for c in sides + rows:
        c.wait()


def start_kernel(
    mv, b_ref, sh_ref, bp_ref, m_ref, node_ref, cond_ref,
    msg_hbm, cm_ref, v0p_ref, bump_ref,
    a_ref, s_ref, t_ref, w_ref, pad_ref, pay_ref, sems,
):
    i, j = where_am_i()
    for n in (4, 5):
        mv.wait(n)
    a_ref[...] = jnp.zeros_like(a_ref)
    ln = iota((1, 128), 1)
    for lr in range(6):
        l = 4 * i + lr - 1
        chunk = lattice_chunk(l)
        ok = (ln // 64 == l % 2) & (l >= 0) & (l < 64)
        nd = node_ref[pl.ds(chunk, 1), :]
        a_ref[lr : lr + 1, :] = jnp.where(ok, nd // 2048 - CELL * l, 0).astype(jnp.float32)
        a_ref[8 + lr : 9 + lr, :] = jnp.where(ok, nd % 2048 - CELL * (ln % 64), 0).astype(jnp.float32)
        a_ref[16 + lr : 17 + lr, :] = jnp.where(ok, cond_ref[pl.ds(chunk, 1), :], 0.0)
    wide = dot_nn(a_ref[...], spread(j))
    maps = [extended_rows([wide[8 * n + lr : 8 * n + lr + 1] for lr in range(6)]) for n in range(3)]
    row = iota((ER, EC), 0)
    here = jnp.where(row < TR, row % CELL, jnp.where(row < TR + 4, row - TR, row - TR + 24))
    cols = iota((ER, EC), 1) % CELL
    hit = (maps[0].astype(jnp.int32) == here) & (maps[1].astype(jnp.int32) == cols)
    cm = jnp.where(hit, maps[2], 0.0)
    cm_ref[...] = cm
    mv.flush(1)
    mv.wait(1)
    here = cm[0:TR, 0:TC]
    rd = 1.0 / (4.0 + sh_ref[...] + here)
    at_bump = jnp.where(here > 0.0, rd, 0.0)
    row, col = iota((TR, TC), 0), iota((TR, TC), 1)
    w_ref[0] = rd
    w_ref[1] = at_bump
    for n, inside in enumerate((row > 0, row < TR - 1, col > 0, col < TC - 1)):
        w_ref[2 + n] = jnp.where(inside, at_bump, 0.0)

    def one(k, c):
        x = b_ref[k] * w_ref[0]
        at = b_ref[k] * w_ref[1]
        down_cells(s_ref, k, at)
        near = pltpu.roll(x, 1, 0) * w_ref[2] + pltpu.roll(x, TR - 1, 0) * w_ref[3]
        near = near + pltpu.roll(x, 1, 1) * w_ref[4] + pltpu.roll(x, TC - 1, 1) * w_ref[5]
        down_cells(t_ref, k, at - near)
        return c

    mv.wait(0)
    lax.fori_loop(0, K, one, 0)
    t_ref[K : K + 8, :] = jnp.zeros((8, 4 * TC), jnp.float32)
    down_cells(t_ref, K, here)
    down_cells(t_ref, K + 1, here * rd)
    bump_ref[...] = gather_bumps(t_ref)
    mv.flush(3)
    mv.wait(2)
    mv.wait(3)
    v0p = padded(pad_ref, dot_nt(bp_ref[...], m_ref[0]))
    v0p_ref[...] = v0p
    mv.flush(2)
    send(msg_hbm, pay_ref, sems, pack(v0p, gather_bumps(s_ref)))


def columns_kernel(mv, g1_ref, edge_ref, w_ref, up_ref, dn_ref, y_ref, ext_ref):
    _, j = where_am_i()
    y_ref[...] = jnp.zeros_like(y_ref)

    @pl.when(j < 7)
    def _():
        y_ref[0:HROWS, :] = g1_ref[jnp.minimum(j + 1, 7), 128 : 128 + HROWS, :]

    @pl.when(j > 0)
    def _():
        y_ref[64 : 64 + HROWS, :] = g1_ref[jnp.maximum(j - 1, 0), 128 : 128 + HROWS, :]

    yt = y_ref[...].T
    lane = iota((TR, 128), 1)
    for k in range(PLANES):
        right = pltpu.roll(yt, (128 - 3 * k) % 128, 1) if k else yt
        left = pltpu.roll(yt, (61 - 3 * k) % 128, 1) if (61 - 3 * k) % 128 else yt
        w_ref[k] = jnp.where(lane < 3, right, jnp.where(lane >= 125, left, 0.0))
    first = iota((8, EC), 0) < 4
    mv.wait(1)
    for k in range(PLANES):
        for side in range(2):
            ext_ref[side, k, :, 0:TC] = edge_ref[k, 8 * side : 8 * side + 8, :]
            ext_ref[side, k, :, TC:EC] = w_ref[k, (TR - 8) * side : (TR - 8) * side + 8, :]
    for p in range(PAIRS):
        q = min(p + PAIRS, PLANES - 1)
        up_ref[p] = jnp.where(first, ext_ref[0, p], pltpu.roll(ext_ref[0, q], 4, 0))
        dn_ref[p] = jnp.where(first, pltpu.roll(ext_ref[1, p], 4, 0), ext_ref[1, q])


def whole_plane(xs_ref, main, w_ref, grp_ref, k):
    xs_ref[0:TR, 0:TC] = main
    xs_ref[0:TR, TC:EC] = w_ref[k]
    xs_ref[TR:ER, :] = grp_ref[k]
    return xs_ref[...]


def package_all(g_ref, v_ref):
    lane = iota((8, 128), 1) // 32

    def one(c, carry):
        lo = jnp.zeros((8, 128), jnp.float32)
        hi = jnp.zeros((8, 128), jnp.float32)
        for m in range(4):
            x = g_ref[4 * c + m]
            lo = jnp.where(lane == m, pltpu.roll(x, 32 * m, 1) if m else x, lo)
            hi = jnp.where(lane == m, pltpu.roll(x, (32 * m - 32) % 128, 1) if m != 1 else x, hi)
        at = pl.ds(pl.multiple_of(128 * c, 128), 128)
        v_ref[0:8, at] = lo
        v_ref[8:16, at] = hi
        return carry

    lax.fori_loop(0, NB // 128, one, 0, unroll=4)


def own_die(g_ref, i, j):
    lane = iota((8, 128), 1)
    halves = []
    for h in range(2):
        out = jnp.zeros((8, 128), jnp.float32)
        for m in range(4):
            x = g_ref[8 * i + 4 * (j % 2) + m]
            shift = 8 * m - (64 + 32 * h + 8 * (j // 2)) + 128
            x = pltpu.roll(x, shift % 128, 1)
            out = jnp.where((lane >= 8 * m) & (lane < 8 * m + 8), x, out)
        halves.append(out)
    return jnp.concatenate(halves, axis=0)


def own_conductance(cond_ref, i, j):
    q = 8 * i + j
    row = cond_ref[pl.ds(q // 4, 1), :]
    return pltpu.roll(row, (128 - 32 * (q % 4)) % 128, 1)


def around(v_ref, x_ref, i):
    ln = iota((K, 128), 1)
    for lr in range(6):
        l = 4 * i + lr - 1
        at = pl.ds(pl.multiple_of(128 * lattice_chunk(l), 128), 128)
        x_ref[K * lr : K * (lr + 1), :] = jnp.where(ln // 64 == l % 2, v_ref[:, at], 0.0)


def coupled(e_ref, k):
    return extended_rows([e_ref[pl.ds(K * lr + k, 1), :] for lr in range(6)])


def beside(x):
    out = pltpu.roll(x, 1, 0) + pltpu.roll(x, ER - 1, 0)
    return out + pltpu.roll(x, 1, 1) + pltpu.roll(x, EC - 1, 1)


def add_dot(r_ref, at, x):
    s = jnp.sum(x, axis=0, keepdims=True)
    r_ref[pl.ds(at, 1), :] = s[:, 0:128] + s[:, 128:256]


def tile(x):
    return x[0:TR, 0:TC]


def edges_kernel(
    mv, sh_ref, w_ref, bot_ref, top_ref, cm_ref, g1_ref, inner_ref,
    w_hbm, grp_ref, bump_ref, pm_ref,
    s_ref, t_ref, sem,
):
    keep = pltpu.make_async_copy(w_ref, w_hbm, sem.at[0])
    keep.start()
    for d in range(8):
        for t in range(4):
            c = 4 * d + t
            pm_ref[:, 128 * c : 128 * (c + 1)] = g1_ref[d, 32 * t : 32 * (t + 1), :]
    mv.flush(3)
    first = iota((8, EC), 0) < 4
    for p in range(PAIRS):
        bot, top = bot_ref[p], top_ref[p]
        grp_ref[p] = jnp.where(first, bot, pltpu.roll(top, 4, 0))
        if p + PAIRS < PLANES:
            grp_ref[p + PAIRS] = jnp.where(first, pltpu.roll(bot, 4, 0), top)
    mv.flush(1)
    for n in (0, 4, 6):
        mv.wait(n)
    inverse = lambda sh, cm: jnp.where(sh > 0.0, 1.0 / (4.0 + sh + cm), 0.0)
    cm = tile(cm_ref)
    at_bump = jnp.where(cm > 0.0, inverse(sh_ref[...], cm), 0.0)
    ends = inverse(grp_ref[K], cm_ref[TR:ER, :])
    above = ends[7:8, 0:TC] * at_bump[0:1]
    below = ends[0:1, 0:TC] * at_bump[TR - 1 : TR]
    lane = iota((TR, 128), 1)
    sides = jnp.where(lane == 0, pltpu.roll(at_bump[:, 128:256], 1, 1), 0.0)
    sides = jnp.where(lane == 127, pltpu.roll(at_bump[:, 0:128], 127, 1), sides)
    sides = sides * inverse(w_ref[K], cm_ref[0:TR, TC:EC])
    s_ref[...] = jnp.zeros_like(s_ref)
    for k in range(K):
        s_ref[k : k + 1, 0:TC] = grp_ref[k, 7:8, 0:TC] * above
        s_ref[k : k + 1, 3 * TC : 4 * TC] = grp_ref[k, 0:1, 0:TC] * below
        z = w_ref[k] * sides
        for lr in range(4):
            t_ref[k : k + 1, 128 * lr : 128 * (lr + 1)] = jnp.sum(
                z[CELL * lr : CELL * (lr + 1)], axis=0, keepdims=True
            )
    at, to = iota((512, 128), 0), iota((512, 128), 1)
    right = (at % 128 == 0) & (to == at // 128 * 8 + 7)
    left = (at % 128 == 127) & (to == at // 128 * 8)
    halo = gather_bumps(s_ref) + dot_nn(t_ref[...], (left | right).astype(jnp.float32))
    bump_ref[0:K, :] = inner_ref[0:K, :] - halo
    bump_ref[K:, :] = inner_ref[K:, :]
    mv.flush(2)
    keep.wait()


def package_kernel(
    step, mv, g_ref, pm_ref, m_ref, cond_ref, bump_ref, const_ref, vp_ref,
    out_ref, vd_ref, y_ref, x_ref, msg_hbm,
    v_ref, pad_ref, pay_ref, sems,
):
    i, j = where_am_i()
    package_all(g_ref, v_ref)
    for n in range(1, 7):
        if n in mv.ins:
            mv.wait(n)
    vp = vp_ref[...]
    y = padded(pad_ref, dot_nt(v_ref[...], pm_ref[...]))
    y = y + own_conductance(cond_ref, i, j) * (vp - own_die(g_ref, i, j))
    y = jnp.where(iota((K, 128), 1) < OWN, y, 0.0)
    out = padded(pad_ref, dot_nt(y[:, 0:OWN], m_ref[0]))
    if step == 2:
        out = out - vp
    vd = bump_ref[0:K, :] - const_ref[K + 1 : K + 2, :] * at_tile(v_ref, i, j)
    y_ref[...] = y
    out_ref[...] = out
    vd_ref[...] = vd
    around(v_ref, x_ref, i)
    for n in range(4):
        mv.flush(n)
    send(msg_hbm, pay_ref, sems, pack(out, vd))


def at_tile(v_ref, i, j):
    ln = iota((K, 128), 1)
    out = jnp.zeros((K, 128), jnp.float32)
    for lr in range(4):
        l = 4 * i + lr
        at = pl.ds(pl.multiple_of(128 * lattice_chunk(l), 128), 128)
        x = pltpu.roll(v_ref[:, at], (8 * lr - 64 * (l % 2) - 8 * j + 256) % 128, 1)
        out = jnp.where((ln >= 8 * lr) & (ln < 8 * lr + 8), x, out)
    return out


def second_kernel(
    mv, b_ref, sh_ref, w_ref, grp_ref, cm_ref, x_ref, bp_ref, v0p_ref, v1p_ref, y1_ref,
    v1_ref, bump_ref, r_ref, rd_ref, dg_ref, cr_ref,
    e_ref, s_ref, pad_ref, xs_ref,
):
    i, j = where_am_i()
    for n in range(1, 10):
        mv.wait(n)
    sh = whole_plane(xs_ref, sh_ref[...], w_ref, grp_ref, K)
    cm = cm_ref[...]
    rd = jnp.where(sh > 0.0, 1.0 / (4.0 + sh + cm), 0.0)
    rd_ref[...] = rd
    cr_ref[...] = cm * rd
    dg_ref[...] = 4.0 + tile(sh) + tile(cm)
    for n in (3, 4, 5):
        mv.flush(n)
    e_ref[...] = dot_nn(x_ref[...], spread(j))

    def one(k, c):
        rd, dg = rd_ref[...], dg_ref[...]
        x0 = whole_plane(xs_ref, b_ref[k], w_ref, grp_ref, k) * rd
        x1 = x0 - (beside(x0) * rd + cr_ref[...] * coupled(e_ref, k))
        v1_ref[k] = x1
        down_cells(s_ref, k, jnp.where(tile(cr_ref) > 0.0, tile(-beside(x1) * rd), 0.0))
        a, b = tile(x0), tile(x1)
        add_dot(r_ref, k, dg * a * a)
        add_dot(r_ref, K + k, dg * a * b)
        add_dot(r_ref, 2 * K + k, dg * b * b)
        return c

    for c in range(CHUNKS):
        mv.wait(0, c)
        lax.fori_loop(4 * c, 4 * c + 4, one, 0)
        mv.flush(0, c)
    bump_ref[...] = gather_bumps(s_ref)
    v0p, v1p, y1 = v0p_ref[...], v1p_ref[...], y1_ref[...]
    bp = padded(pad_ref, bp_ref[...])
    r_ref[0:K, :] += v0p * bp
    r_ref[K : 2 * K, :] += v0p * y1
    r_ref[2 * K : 3 * K, :] += v1p * y1
    mv.flush(2)


def third_kernel(
    mv, v1_ref, rd_ref, dg_ref, cr_ref, x_ref, wp_ref, y1_ref, y2_ref, ra_ref,
    wt_ref, r_ref,
    e_ref,
):
    i, j = where_am_i()
    for n in range(1, 9):
        mv.wait(n)
    e_ref[...] = dot_nn(x_ref[...], spread(j))
    r_ref[6 * K :, :] = jnp.zeros((2 * K, 128), jnp.float32)
    r_ref[0 : 3 * K, :] = ra_ref[...]

    def one(k, c):
        dg = dg_ref[...]
        x1 = v1_ref[k]
        w = -(beside(x1) * rd_ref[...] + cr_ref[...] * coupled(e_ref, k))
        a, b = tile(x1), tile(w)
        wt_ref[k] = b
        add_dot(r_ref, 3 * K + k, dg * a * b)
        add_dot(r_ref, 4 * K + k, dg * b * b)
        add_dot(r_ref, 5 * K + k, dg * b * (b - tile(beside(w)) * tile(rd_ref)))
        return c

    for c in range(CHUNKS):
        mv.wait(0, c)
        lax.fori_loop(4 * c, 4 * c + 4, one, 0)
        mv.flush(0, c)
    wp, y1, y2 = wp_ref[...], y1_ref[...], y2_ref[...]
    r_ref[3 * K : 4 * K, :] += wp * y1
    r_ref[4 * K : 5 * K, :] += wp * (y2 - y1)


def fourth_kernel(
    mv, g_ref, pm_ref, cond_ref, const_ref, wp_ref, wd_ref, ra_ref, v1_hbm, w_hbm,
    msg_ref, v1_ref, w_ref,
    v_ref, pad_ref, r_ref, sems,
):
    i, j = where_am_i()
    loads = [
        pltpu.make_async_copy(v1_hbm.at[:, 0:TR, 0:TC], v1_ref, sems.at[0]),
        pltpu.make_async_copy(w_hbm, w_ref, sems.at[1]),
    ]
    for c in loads:
        c.start()
    package_all(g_ref, v_ref)
    for n in range(1, 6):
        mv.wait(n)
    wp = wp_ref[...]
    y = padded(pad_ref, dot_nt(v_ref[...], pm_ref[...]))
    y = y + own_conductance(cond_ref, i, j) * (wp - own_die(g_ref, i, j))
    y = jnp.where(iota((K, 128), 1) < OWN, y, 0.0)
    r_ref[...] = ra_ref[...]
    r_ref[5 * K : 6 * K, :] += wp * y - const_ref[K : K + 1, :] * wd_ref[...] * at_tile(v_ref, i, j)
    sums = dot_nt(jnp.ones((8, 128), jnp.float32), r_ref[...])

    def one(d, c):
        msg_ref[d] = sums[0:1]
        return c

    lax.fori_loop(0, msg_ref.shape[0], one, 0, unroll=8)
    for c in loads:
        c.wait()


def last_kernel(
    mv, g_ref, b_ref, rd_ref, v1_ref, v2_ref, v0p_ref, v1p_ref, v2p_ref,
    xd_ref, xp_ref, c_ref,
):
    total = jnp.sum(g_ref[...], axis=0)
    total = jnp.broadcast_to(total, (8, 128))
    m = [pltpu.roll(total, (128 - K * n) % 128, 1) if n else total for n in range(6)]
    g00, g01, g02, g11, g12, g22 = m[1], m[2], m[3], m[2] + m[3], m[3] + m[4], m[5]
    f1, f2 = g01 / g00, g02 / g00
    a11, a12, h1 = g11 - f1 * g01, g12 - f1 * g02, g00 - f1 * m[0]
    a22, h2 = g22 - f2 * g02, g01 - g00 - f2 * m[0]
    f3 = a12 / a11
    c2 = (h2 - f3 * h1) / (a22 - f3 * a12)
    c1 = (h1 - a12 * c2) / a11
    c0 = (m[0] - g01 * c1 - g02 * c2) / g00
    rd = tile(rd_ref)
    at = iota((K, 128), 0) == iota((K, 128), 1)
    cols = []
    for n, c in enumerate((c0, c1, c2)):
        col = jnp.sum(jnp.where(at, c[0:1], 0.0), axis=1, keepdims=True)
        cols.append(col)
        c_ref[n] = jnp.broadcast_to(col, (K, TC))
    xp = cols[0] * v0p_ref[...] + cols[1] * v1p_ref[...] + cols[2] * v2p_ref[...]
    xp_ref[...] = xp[:, 0:OWN]

    def one(k, carry):
        c0, c1, c2 = (c_ref[n, pl.ds(k, 1), :] for n in range(3))
        xd_ref[k] = (c0 * b_ref[k]) * rd + c1 * v1_ref[k] + c2 * v2_ref[k]
        return carry

    for c in range(CHUNKS):
        lax.fori_loop(4 * c, 4 * c + 4, one, 0)
        mv.flush(0, c)


def f32(*shape):
    return jax.ShapeDtypeStruct(shape, jnp.float32)


def vm(*shape):
    return pltpu.VMEM(shape, jnp.float32)


CHUNKS = 4


class Moves:
    def __init__(self):
        self.ins, self.outs, self.pending = {}, {}, []

    def wait(self, n, chunk=None):
        for c in [chunk] if chunk is not None else range(len(self.ins[n])):
            self.ins[n][c].wait()
            self.ins[n][c] = None

    def flush(self, n, chunk=None):
        for c in [chunk] if chunk is not None else range(len(self.outs[n])):
            self.outs[n][c].start()
            self.pending.append(self.outs[n][c])


def parts(ref, mode):
    if mode == "h":
        return [ref]
    step = ref.shape[0] // CHUNKS
    return [ref.at[step * c : step * (c + 1)] for c in range(CHUNKS)]


def call(kernel, ins, outs, scratch, limit=14, **kw):
    imode, omode = [m for _, m in ins], [m for _, m in outs]
    moved = [jax.ShapeDtypeStruct(x.shape, x.dtype) for x, m in ins + outs if m in "hc"]
    count = sum({"h": 1, "c": CHUNKS}.get(m, 0) for m in imode + omode)

    def wrapped(*refs):
        ni, no, nm = len(ins), len(outs), len(moved)
        hbm, bufs, sems, own = refs[: ni + no], list(refs[ni + no :][:nm]), refs[ni + no + nm], refs[ni + no + nm + 1 :]
        mv, given, sem = Moves(), [], 0
        for n, (ref, mode) in enumerate(zip(hbm, imode + omode)):
            if mode not in "hc":
                given.append(ref)
                continue
            buf = bufs.pop(0)
            given.append(buf)
            copies = []
            for x, y in zip(parts(ref, mode), parts(buf, mode)):
                x, y = (x, y) if n < ni else (y, x)
                copies.append(pltpu.make_async_copy(x, y, sems.at[sem]))
                sem += 1
            (mv.ins if n < ni else mv.outs)[n if n < ni else n - ni] = copies
        for copies in sorted(mv.ins.values(), key=len):
            for c in copies:
                c.start()
        kernel(mv, *given, *own)
        for copies in mv.ins.values():
            assert all(c is None for c in copies)
        for c in mv.pending:
            c.wait()

    space = lambda m: pl.BlockSpec(memory_space=pltpu.VMEM if m == "v" else pltpu.HBM)
    return pl.pallas_call(
        wrapped,
        out_shape=tuple(x if m == "v" else pltpu.HBM(x.shape, x.dtype) for x, m in outs),
        in_specs=[space(m) for m in imode],
        out_specs=tuple(space(m) for m in omode),
        scratch_shapes=[pltpu.VMEM(x.shape, x.dtype) for x in moved]
        + [pltpu.SemaphoreType.DMA((max(count, 1),))] + scratch,
        compiler_params=pltpu.CompilerParams(vmem_limit_bytes=limit << 20),
        name=getattr(kernel, "func", kernel).__name__,
        **kw,
    )(*[x if m == "v" else pltpu.with_memory_space_constraint(x, pltpu.HBM) for x, m in ins])


def swapped(x, axes):
    return lax.all_to_all(x, axes, 0, 0, tiled=True)


def body(
    die_current, die_shunt, pkg_current, pkg_matrix, pkg_block_inv, bump_node, bump_conductance
):
    nodes = bump_node.reshape(NB // 128, 128)
    cond = bump_conductance.reshape(NB // 128, 128)
    b, sh, bp, m = die_current, die_shunt, pkg_current, pkg_block_inv
    gathered, small, ext, die = f32(128, 8, 128), f32(K, 128), f32(K, ER, EC), f32(K, TR, TC)
    lattice = f32(6 * K, 128)
    payload = [vm(128 // SENDS, 8, 128), pltpu.SemaphoreType.DMA((SENDS,))]
    msg1, edge = call(
        load_kernel,
        [(b, "c"), (sh, "h"), (pkg_matrix.reshape(8, OWN, 512), "h")],
        [(f32(8, 128 + HROWS, 128), "r"), (f32(PLANES, 16, TC), "h")],
        [vm(128, 128), pltpu.SemaphoreType.DMA((6,))],
    )
    g1 = swapped(msg1, COL)
    msg, cm, v0p, bump1 = call(
        start_kernel,
        [(b, "h"), (sh, "h"), (bp, "h"), (m, "h"), (nodes, "h"), (cond, "h")],
        [(gathered, "r"), (f32(ER, EC), "h"), (small, "h"), (f32(K + 8, 128), "h")],
        [vm(24, 128), vm(K, 4 * TC), vm(K + 8, 4 * TC), vm(6, TR, TC), vm(K, 128)] + payload,
    )
    g = swapped(msg, ROW_COL)
    side, up, dn = call(
        columns_kernel,
        [(g1, "v"), (edge, "h")],
        [(f32(PLANES, TR, 128), "v"), (f32(PAIRS, 8, EC), "v"), (f32(PAIRS, 8, EC), "v")],
        [vm(128, 128), vm(2, PLANES, 8, EC)],
    )
    n = lax.axis_size(ROW)
    bot = lax.ppermute(up, ROW, [(r + 1, r) for r in range(n - 1)])
    top = lax.ppermute(dn, ROW, [(r, r + 1) for r in range(n - 1)])
    side, grp, bump1, pm = call(
        edges_kernel,
        [(sh, "h"), (side, "v"), (bot, "v"), (top, "v"), (cm, "h"), (g1, "v"), (bump1, "h")],
        [
            (f32(PLANES, TR, 128), "r"), (f32(PLANES, 8, EC), "h"), (f32(K + 8, 128), "h"),
            (f32(OWN, NB), "h"),
        ],
        [vm(K, 4 * TC), vm(K, 512), pltpu.SemaphoreType.DMA((1,))],
    )
    step = [vm(K, NB), vm(K, 128)] + payload
    results = [(small, "h"), (small, "h"), (small, "h"), (lattice, "h"), (gathered, "r")]
    v1p, _, y1, near, msg = call(
        functools.partial(package_kernel, 1),
        [(g, "v"), (pm, "h"), (m, "h"), (cond, "h"), (bump1, "h"), (bump1, "h"), (v0p, "h")],
        results,
        step,
    )
    g = swapped(msg, ROW_COL)
    v1, bump2, r, rd, dg, cr = call(
        second_kernel,
        [(b, "c")] + [(x, "h") for x in (sh, side, grp, cm, near, bp, v0p, v1p, y1)],
        [
            (ext, "c"), (small, "v"), (f32(3 * K, 128), "h"), (f32(ER, EC), "h"),
            (f32(TR, TC), "h"), (f32(ER, EC), "h"),
        ],
        [vm(6 * K, EC), vm(K, 4 * TC), vm(K, 128), vm(ER, EC)],
    )
    wp, wd, y2, near, msg = call(
        functools.partial(package_kernel, 2),
        [(g, "v"), (pm, "h"), (m, "h"), (cond, "h"), (bump2, "v"), (bump1, "h"), (v1p, "h")],
        results,
        step,
    )
    g = swapped(msg, ROW_COL)
    w, r = call(
        third_kernel,
        [(v1, "c")] + [(x, "h") for x in (rd, dg, cr, near, wp, y1, y2, r)],
        [(die, "c"), (f32(128, 128), "v")],
        [vm(6 * K, EC)],
    )
    msg, v1, w = call(
        fourth_kernel,
        [(g, "v")] + [(x, "h") for x in (pm, cond, bump1, wp, wd)] + [(r, "v"), (v1, "r"), (w, "r")],
        [(f32(128, 1, 128), "v"), (die, "v"), (die, "v")],
        [vm(K, NB), vm(K, 128), vm(128, 128), pltpu.SemaphoreType.DMA((2,))],
    )
    g = swapped(msg, ROW_COL)
    return call(
        last_kernel,
        [(x, "v") for x in (g, b, rd, v1, w, v0p, v1p, wp)],
        [(die, "c"), (f32(K, OWN), "v")],
        [vm(3, K, TC)],
    )


def solution(mesh):
    torus = Mesh(mesh.devices.reshape(2, 4, 2, 4, 2), ROW_COL)
    placed = (
        P(None, ROW, COL),
        P(ROW, COL),
        P(None, ROW_COL),
        P(ROW, COL),
        P(ROW_COL, None, None),
        P(),
        P(),
    )
    return jax.shard_map(
        body,
        mesh=torus,
        in_specs=placed,
        out_specs=(P(None, ROW, COL), P(None, ROW_COL)),
        check_vma=False,
    )
```

```python
import functools

import jax
import jax.numpy as jnp
from jax import lax
from jax.experimental import pallas as pl
from jax.experimental.pallas import tpu as pltpu
from jax.sharding import Mesh
from jax.sharding import PartitionSpec as P

ROW = ("row_0", "row_1", "row_2")
COL = ("col_0", "col_1")
ROW_COL = ("row_0", "row_1", "row_2", "col_0", "col_1")

K = 16
TR, TC = 128, 256
ER, EC = 136, 384
CELL = 32
PLANES = K + 1
PAIRS = 9
HROWS = 56
OWN = 32
NB = 4096
HI = lax.Precision.HIGHEST


def iota(shape, dim):
    return lax.broadcasted_iota(jnp.int32, shape, dim)


def where_am_i():
    i = (lax.axis_index("row_0") * 4 + lax.axis_index("row_1")) * 2 + lax.axis_index("row_2")
    j = lax.axis_index("col_0") * 2 + lax.axis_index("col_1")
    return i, j


def dot_nt(a, b):
    return lax.dot_general(
        a, b, (((1,), (1,)), ((), ())), precision=HI, preferred_element_type=jnp.float32
    )


def dot_nn(a, b):
    return jnp.dot(a, b, precision=HI, preferred_element_type=jnp.float32)


def spread(j):
    group = iota((128, EC), 1) // CELL
    cell = jnp.where(group <= 8, 8 * j + group, jnp.where(group == 11, 8 * j - 1, -5))
    return (iota((128, EC), 0) % 64 == cell).astype(jnp.float32)


def lattice_chunk(l):
    return jnp.clip(l // 2, 0, NB // 128 - 1)


def extended_rows(parts):
    body = [jnp.broadcast_to(p, (CELL, EC)) for p in parts[1:5]]
    edge = jnp.where(iota((8, EC), 0) < 4, parts[5], parts[0])
    return jnp.concatenate(body + [edge], axis=0)


def padded(scr, x):
    scr[...] = jnp.zeros_like(scr)
    scr[:, 0 : x.shape[1]] = x
    return scr[...]


def pack(vp, vd):
    lane = iota((8, 128), 1)
    hi = pltpu.roll(vp[8:16], 32, 1)
    out = jnp.where(lane < 32, vp[0:8], hi)
    out = jnp.where(lane < 64, out, pltpu.roll(vd[0:8], 64, 1))
    return jnp.where(lane < 96, out, pltpu.roll(vd[8:16], 96, 1))


def pack_package(vp):
    lane = iota((4, 128), 1)
    out = vp[0:4]
    for m in range(1, 4):
        out = jnp.where(lane // 32 == m, pltpu.roll(vp, 32 * m, 1)[4 * m : 4 * m + 4], out)
    return out


def gather_bumps(s_ref):
    at = iota((4 * TC, 128), 0)
    pick = (at // TC * 8 + at % TC // CELL == iota((4 * TC, 128), 1)).astype(jnp.float32)
    return dot_nn(s_ref[...], pick)


def down_cells(s_ref, k, z):
    for lr in range(4):
        rows = z[CELL * lr : CELL * (lr + 1)]
        s_ref[pl.ds(k, 1), TC * lr : TC * (lr + 1)] = jnp.sum(rows, axis=0, keepdims=True)


SENDS = 8


def send(msg_hbm, pay_ref, sems, pay):
    n = pay_ref.shape[0]
    for d in range(n):
        pay_ref[d] = pay
    copies = [
        pltpu.make_async_copy(pay_ref, msg_hbm.at[n * c : n * (c + 1)], sems.at[c]) for c in range(SENDS)
    ]
    for c in copies:
        c.start()
    for c in copies:
        c.wait()


def load_kernel(mv, b_ref, sh_ref, p_ref, msg_hbm, edge_ref, z_ref, sems):
    _, j = where_am_i()
    lane = iota((TR, 128), 1)
    z = jnp.zeros((TR, 128), jnp.float32)
    mv.wait(1)
    for k in [K] + list(range(K)):
        if k < K and k % 4 == 0:
            mv.wait(0, k // 4)
        src = b_ref.at[k] if k < K else sh_ref
        lo = pltpu.roll(src[:, 0:128], 3 * k, 1) if k else src[:, 0:128]
        up = pltpu.roll(src[:, 128:256], (64 + 3 * k - 125) % 128, 1)
        z = jnp.where((lane >= 3 * k) & (lane < 3 * k + 3), lo, z)
        z = jnp.where((lane >= 64 + 3 * k) & (lane < 67 + 3 * k), up, z)
        edge_ref[k, 0:8, :] = src[0:8, :]
        edge_ref[k, 8:16, :] = src[TR - 8 : TR, :]
    mv.flush(1)
    mv.wait(2)
    rows = [
        pltpu.make_async_copy(
            p_ref.at[:, :, 128 * t : 128 * (t + 1)],
            msg_hbm.at[:, 32 * t : 32 * (t + 1), :],
            sems.at[t],
        )
        for t in range(4)
    ]
    for c in rows:
        c.start()
    z_ref[...] = z.T
    side = lambda at, to, n: pltpu.make_async_copy(
        z_ref.at[at : at + HROWS, :], msg_hbm.at[to, 128 : 128 + HROWS, :], sems.at[n]
    )
    sides = [side(0, jnp.maximum(j - 1, 0), 4), side(64, jnp.minimum(j + 1, 7), 5)]
    for c in sides:
        c.start()
    for c in sides + rows:
        c.wait()


def start_kernel(
    mv, b_ref, sh_ref, bp_ref, m_ref, node_ref, cond_ref,
    msg_hbm, cm_ref, v0p_ref, bump_ref,
    a_ref, s_ref, t_ref, w_ref, pad_ref, pay_ref, sems,
):
    i, j = where_am_i()
    for n in (4, 5):
        mv.wait(n)
    a_ref[...] = jnp.zeros_like(a_ref)
    ln = iota((1, 128), 1)
    for lr in range(6):
        l = 4 * i + lr - 1
        chunk = lattice_chunk(l)
        ok = (ln // 64 == l % 2) & (l >= 0) & (l < 64)
        nd = node_ref[pl.ds(chunk, 1), :]
        a_ref[lr : lr + 1, :] = jnp.where(ok, nd // 2048 - CELL * l, 0).astype(jnp.float32)
        a_ref[8 + lr : 9 + lr, :] = jnp.where(ok, nd % 2048 - CELL * (ln % 64), 0).astype(jnp.float32)
        a_ref[16 + lr : 17 + lr, :] = jnp.where(ok, cond_ref[pl.ds(chunk, 1), :], 0.0)
    wide = dot_nn(a_ref[...], spread(j))
    maps = [extended_rows([wide[8 * n + lr : 8 * n + lr + 1] for lr in range(6)]) for n in range(3)]
    row = iota((ER, EC), 0)
    here = jnp.where(row < TR, row % CELL, jnp.where(row < TR + 4, row - TR, row - TR + 24))
    cols = iota((ER, EC), 1) % CELL
    hit = (maps[0].astype(jnp.int32) == here) & (maps[1].astype(jnp.int32) == cols)
    cm = jnp.where(hit, maps[2], 0.0)
    cm_ref[...] = cm
    mv.flush(1)
    mv.wait(1)
    here = cm[0:TR, 0:TC]
    rd = 1.0 / (4.0 + sh_ref[...] + here)
    at_bump = jnp.where(here > 0.0, rd, 0.0)
    row, col = iota((TR, TC), 0), iota((TR, TC), 1)
    w_ref[0] = rd
    w_ref[1] = at_bump
    for n, inside in enumerate((row > 0, row < TR - 1, col > 0, col < TC - 1)):
        w_ref[2 + n] = jnp.where(inside, at_bump, 0.0)

    def one(k, c):
        x = b_ref[k] * w_ref[0]
        at = b_ref[k] * w_ref[1]
        down_cells(s_ref, k, at)
        near = pltpu.roll(x, 1, 0) * w_ref[2] + pltpu.roll(x, TR - 1, 0) * w_ref[3]
        near = near + pltpu.roll(x, 1, 1) * w_ref[4] + pltpu.roll(x, TC - 1, 1) * w_ref[5]
        down_cells(t_ref, k, at - near)
        return c

    mv.wait(0)
    lax.fori_loop(0, K, one, 0)
    t_ref[K : K + 8, :] = jnp.zeros((8, 4 * TC), jnp.float32)
    down_cells(t_ref, K, here)
    down_cells(t_ref, K + 1, here * rd)
    bump_ref[...] = gather_bumps(t_ref)
    mv.flush(3)
    mv.wait(2)
    mv.wait(3)
    v0p = padded(pad_ref, dot_nt(bp_ref[...], m_ref[0]))
    v0p_ref[...] = v0p
    mv.flush(2)
    send(msg_hbm, pay_ref, sems, pack(v0p, gather_bumps(s_ref)))


def columns_kernel(mv, g1_ref, edge_ref, w_ref, up_ref, dn_ref, y_ref, ext_ref):
    _, j = where_am_i()
    y_ref[...] = jnp.zeros_like(y_ref)

    @pl.when(j < 7)
    def _():
        y_ref[0:HROWS, :] = g1_ref[jnp.minimum(j + 1, 7), 128 : 128 + HROWS, :]

    @pl.when(j > 0)
    def _():
        y_ref[64 : 64 + HROWS, :] = g1_ref[jnp.maximum(j - 1, 0), 128 : 128 + HROWS, :]

    yt = y_ref[...].T
    lane = iota((TR, 128), 1)
    for k in range(PLANES):
        right = pltpu.roll(yt, (128 - 3 * k) % 128, 1) if k else yt
        left = pltpu.roll(yt, (61 - 3 * k) % 128, 1) if (61 - 3 * k) % 128 else yt
        w_ref[k] = jnp.where(lane < 3, right, jnp.where(lane >= 125, left, 0.0))
    first = iota((8, EC), 0) < 4
    mv.wait(1)
    for k in range(PLANES):
        for side in range(2):
            ext_ref[side, k, :, 0:TC] = edge_ref[k, 8 * side : 8 * side + 8, :]
            ext_ref[side, k, :, TC:EC] = w_ref[k, (TR - 8) * side : (TR - 8) * side + 8, :]
    for p in range(PAIRS):
        q = min(p + PAIRS, PLANES - 1)
        up_ref[p] = jnp.where(first, ext_ref[0, p], pltpu.roll(ext_ref[0, q], 4, 0))
        dn_ref[p] = jnp.where(first, pltpu.roll(ext_ref[1, p], 4, 0), ext_ref[1, q])


def whole_plane(xs_ref, main, w_ref, grp_ref, k):
    xs_ref[0:TR, 0:TC] = main
    xs_ref[0:TR, TC:EC] = w_ref[k]
    xs_ref[TR:ER, :] = grp_ref[k]
    return xs_ref[...]


def package_all(g_ref, v_ref):
    lane = iota((8, 128), 1) // 32

    def one(c, carry):
        lo = jnp.zeros((8, 128), jnp.float32)
        hi = jnp.zeros((8, 128), jnp.float32)
        for m in range(4):
            x = g_ref[4 * c + m]
            lo = jnp.where(lane == m, pltpu.roll(x, 32 * m, 1) if m else x, lo)
            hi = jnp.where(lane == m, pltpu.roll(x, (32 * m - 32) % 128, 1) if m != 1 else x, hi)
        at = pl.ds(pl.multiple_of(128 * c, 128), 128)
        v_ref[0:8, at] = lo
        v_ref[8:16, at] = hi
        return carry

    lax.fori_loop(0, NB // 128, one, 0, unroll=4)


def package_only(g_ref, v_ref):
    lane = iota((4, 128), 1) // 32

    def one(c, carry):
        xs = [g_ref[4 * c + d] for d in range(4)]
        at = pl.ds(pl.multiple_of(128 * c, 128), 128)
        for m in range(4):
            out = xs[m]
            for d in range(4):
                if d != m:
                    out = jnp.where(lane == d, pltpu.roll(xs[d], (32 * (d - m)) % 128, 1), out)
            v_ref[4 * m : 4 * m + 4, at] = out
        return carry

    lax.fori_loop(0, NB // 128, one, 0, unroll=4)


def own_die(g_ref, i, j):
    lane = iota((8, 128), 1)
    halves = []
    for h in range(2):
        out = jnp.zeros((8, 128), jnp.float32)
        for m in range(4):
            x = g_ref[8 * i + 4 * (j % 2) + m]
            shift = 8 * m - (64 + 32 * h + 8 * (j // 2)) + 128
            x = pltpu.roll(x, shift % 128, 1)
            out = jnp.where((lane >= 8 * m) & (lane < 8 * m + 8), x, out)
        halves.append(out)
    return jnp.concatenate(halves, axis=0)


def own_conductance(cond_ref, i, j):
    q = 8 * i + j
    row = cond_ref[pl.ds(q // 4, 1), :]
    return pltpu.roll(row, (128 - 32 * (q % 4)) % 128, 1)


def around(v_ref, x_ref, i):
    ln = iota((K, 128), 1)
    for lr in range(6):
        l = 4 * i + lr - 1
        at = pl.ds(pl.multiple_of(128 * lattice_chunk(l), 128), 128)
        x_ref[K * lr : K * (lr + 1), :] = jnp.where(ln // 64 == l % 2, v_ref[:, at], 0.0)


def coupled(e_ref, k):
    return extended_rows([e_ref[pl.ds(K * lr + k, 1), :] for lr in range(6)])


def beside(x):
    out = pltpu.roll(x, 1, 0) + pltpu.roll(x, ER - 1, 0)
    return out + pltpu.roll(x, 1, 1) + pltpu.roll(x, EC - 1, 1)


def add_dot(r_ref, at, x):
    s = jnp.sum(x, axis=0, keepdims=True)
    r_ref[pl.ds(at, 1), :] = s[:, 0:128] + s[:, 128:256]


def tile(x):
    return x[0:TR, 0:TC]


def edges_kernel(
    mv, sh_ref, w_ref, bot_ref, top_ref, cm_ref, g1_ref, inner_ref,
    w_hbm, grp_ref, bump_ref, pm_ref,
    s_ref, t_ref, sem,
):
    keep = pltpu.make_async_copy(w_ref, w_hbm, sem.at[0])
    keep.start()
    for d in range(8):
        for t in range(4):
            c = 4 * d + t
            pm_ref[:, 128 * c : 128 * (c + 1)] = g1_ref[d, 32 * t : 32 * (t + 1), :]
    mv.flush(3)
    first = iota((8, EC), 0) < 4
    for p in range(PAIRS):
        bot, top = bot_ref[p], top_ref[p]
        grp_ref[p] = jnp.where(first, bot, pltpu.roll(top, 4, 0))
        if p + PAIRS < PLANES:
            grp_ref[p + PAIRS] = jnp.where(first, pltpu.roll(bot, 4, 0), top)
    mv.flush(1)
    for n in (0, 4, 6):
        mv.wait(n)
    inverse = lambda sh, cm: jnp.where(sh > 0.0, 1.0 / (4.0 + sh + cm), 0.0)
    cm = tile(cm_ref)
    at_bump = jnp.where(cm > 0.0, inverse(sh_ref[...], cm), 0.0)
    ends = inverse(grp_ref[K], cm_ref[TR:ER, :])
    above = ends[7:8, 0:TC] * at_bump[0:1]
    below = ends[0:1, 0:TC] * at_bump[TR - 1 : TR]
    lane = iota((TR, 128), 1)
    sides = jnp.where(lane == 0, pltpu.roll(at_bump[:, 128:256], 1, 1), 0.0)
    sides = jnp.where(lane == 127, pltpu.roll(at_bump[:, 0:128], 127, 1), sides)
    sides = sides * inverse(w_ref[K], cm_ref[0:TR, TC:EC])
    s_ref[...] = jnp.zeros_like(s_ref)
    for k in range(K):
        s_ref[k : k + 1, 0:TC] = grp_ref[k, 7:8, 0:TC] * above
        s_ref[k : k + 1, 3 * TC : 4 * TC] = grp_ref[k, 0:1, 0:TC] * below
        z = w_ref[k] * sides
        for lr in range(4):
            t_ref[k : k + 1, 128 * lr : 128 * (lr + 1)] = jnp.sum(
                z[CELL * lr : CELL * (lr + 1)], axis=0, keepdims=True
            )
    at, to = iota((512, 128), 0), iota((512, 128), 1)
    right = (at % 128 == 0) & (to == at // 128 * 8 + 7)
    left = (at % 128 == 127) & (to == at // 128 * 8)
    halo = gather_bumps(s_ref) + dot_nn(t_ref[...], (left | right).astype(jnp.float32))
    bump_ref[0:K, :] = inner_ref[0:K, :] - halo
    bump_ref[K:, :] = inner_ref[K:, :]
    mv.flush(2)
    keep.wait()


def package_kernel(
    step, mv, g_ref, pm_ref, m_ref, cond_ref, bump_ref, const_ref, vp_ref,
    out_ref, vd_ref, y_ref, x_ref, msg_hbm,
    v_ref, pad_ref, pay_ref, sems,
):
    i, j = where_am_i()
    package_all(g_ref, v_ref)
    for n in range(1, 7):
        if n in mv.ins:
            mv.wait(n)
    vp = vp_ref[...]
    y = padded(pad_ref, dot_nt(v_ref[...], pm_ref[...]))
    y = y + own_conductance(cond_ref, i, j) * (vp - own_die(g_ref, i, j))
    y = jnp.where(iota((K, 128), 1) < OWN, y, 0.0)
    out = padded(pad_ref, dot_nt(y[:, 0:OWN], m_ref[0]))
    if step == 2:
        out = out - vp
    vd = bump_ref[0:K, :] - const_ref[K + 1 : K + 2, :] * at_tile(v_ref, i, j)
    y_ref[...] = y
    out_ref[...] = out
    vd_ref[...] = vd
    around(v_ref, x_ref, i)
    for n in range(4):
        mv.flush(n)
    send(msg_hbm, pay_ref, sems, pack(out, vd) if step == 1 else pack_package(out))


def at_tile(v_ref, i, j):
    ln = iota((K, 128), 1)
    out = jnp.zeros((K, 128), jnp.float32)
    for lr in range(4):
        l = 4 * i + lr
        at = pl.ds(pl.multiple_of(128 * lattice_chunk(l), 128), 128)
        x = pltpu.roll(v_ref[:, at], (8 * lr - 64 * (l % 2) - 8 * j + 256) % 128, 1)
        out = jnp.where((ln >= 8 * lr) & (ln < 8 * lr + 8), x, out)
    return out


def second_kernel(
    mv, b_ref, sh_ref, w_ref, grp_ref, cm_ref, x_ref, bp_ref, v0p_ref, v1p_ref, y1_ref,
    v1_ref, bump_ref, r_ref, rd_ref, dg_ref, cr_ref, next_ref,
    e_ref, s_ref, pad_ref, xs_ref,
):
    i, j = where_am_i()
    for n in range(1, 10):
        mv.wait(n)
    sh = whole_plane(xs_ref, sh_ref[...], w_ref, grp_ref, K)
    cm = cm_ref[...]
    rd = jnp.where(sh > 0.0, 1.0 / (4.0 + sh + cm), 0.0)
    rd_ref[...] = rd
    cr_ref[...] = cm * rd
    dg_ref[...] = 4.0 + tile(sh) + tile(cm)
    for n in (3, 4, 5):
        mv.flush(n)
    e_ref[...] = dot_nn(x_ref[...], spread(j))

    def one(k, c):
        rd, dg = rd_ref[...], dg_ref[...]
        x0 = whole_plane(xs_ref, b_ref[k], w_ref, grp_ref, k) * rd
        x1 = x0 - (beside(x0) * rd + cr_ref[...] * coupled(e_ref, k))
        v1_ref[k] = tile(x1)
        near = -beside(x1) * rd
        next_ref[k] = near
        down_cells(s_ref, k, jnp.where(tile(cr_ref) > 0.0, tile(near), 0.0))
        a, b = tile(x0), tile(x1)
        add_dot(r_ref, k, dg * a * a)
        add_dot(r_ref, K + k, dg * a * b)
        add_dot(r_ref, 2 * K + k, dg * b * b)
        return c

    for c in range(CHUNKS):
        mv.wait(0, c)
        lax.fori_loop(4 * c, 4 * c + 4, one, 0)
        mv.flush(0, c)
        mv.flush(6, c)
    bump_ref[...] = gather_bumps(s_ref)
    v0p, v1p, y1 = v0p_ref[...], v1p_ref[...], y1_ref[...]
    bp = padded(pad_ref, bp_ref[...])
    r_ref[0:K, :] += v0p * bp
    r_ref[K : 2 * K, :] += v0p * y1
    r_ref[2 * K : 3 * K, :] += v1p * y1
    mv.flush(2)


def third_kernel(
    mv, next_ref, v1_ref, rd_ref, dg_ref, cr_ref, x_ref, wp_ref, y1_ref, y2_ref, ra_ref,
    wt_ref, r_ref,
    e_ref,
):
    i, j = where_am_i()
    for n in range(2, 10):
        mv.wait(n)
    e_ref[...] = dot_nn(x_ref[...], spread(j))
    r_ref[6 * K :, :] = jnp.zeros((2 * K, 128), jnp.float32)
    r_ref[0 : 3 * K, :] = ra_ref[...]

    def one(k, c):
        dg = dg_ref[...]
        w = next_ref[k] - cr_ref[...] * coupled(e_ref, k)
        a, b = v1_ref[k], tile(w)
        wt_ref[k] = b
        add_dot(r_ref, 3 * K + k, dg * a * b)
        add_dot(r_ref, 4 * K + k, dg * b * b)
        add_dot(r_ref, 5 * K + k, dg * b * (b - tile(beside(w)) * tile(rd_ref)))
        return c

    for c in range(CHUNKS):
        mv.wait(0, c)
        mv.wait(1, c)
        lax.fori_loop(4 * c, 4 * c + 4, one, 0)
        mv.flush(0, c)
    wp, y1, y2 = wp_ref[...], y1_ref[...], y2_ref[...]
    r_ref[3 * K : 4 * K, :] += wp * y1
    r_ref[4 * K : 5 * K, :] += wp * (y2 - y1)


def fourth_kernel(
    mv, g_ref, pm_ref, cond_ref, const_ref, wp_ref, wd_ref, ra_ref, v1_hbm, w_hbm,
    msg_ref, v1_ref, w_ref,
    v_ref, pad_ref, r_ref, sems,
):
    i, j = where_am_i()
    loads = [
        pltpu.make_async_copy(v1_hbm, v1_ref, sems.at[0]),
        pltpu.make_async_copy(w_hbm, w_ref, sems.at[1]),
    ]
    for c in loads:
        c.start()
    package_only(g_ref, v_ref)
    for n in range(1, 6):
        mv.wait(n)
    wp = wp_ref[...]
    y = padded(pad_ref, dot_nt(v_ref[...], pm_ref[...])) + own_conductance(cond_ref, i, j) * wp
    y = jnp.where(iota((K, 128), 1) < OWN, y, 0.0)
    r_ref[...] = ra_ref[...]
    both = const_ref[K : K + 1, :] * wd_ref[...] * at_tile(v_ref, i, j)
    r_ref[5 * K : 6 * K, :] += wp * y - 2.0 * both
    sums = dot_nt(jnp.ones((8, 128), jnp.float32), r_ref[...])

    def one(d, c):
        msg_ref[d] = sums[0:1]
        return c

    lax.fori_loop(0, msg_ref.shape[0], one, 0, unroll=8)
    for c in loads:
        c.wait()


def last_kernel(
    mv, g_ref, b_ref, rd_ref, v1_ref, v2_ref, v0p_ref, v1p_ref, v2p_ref,
    xd_ref, xp_ref, c_ref,
):
    total = jnp.sum(g_ref[...], axis=0)
    total = jnp.broadcast_to(total, (8, 128))
    m = [pltpu.roll(total, (128 - K * n) % 128, 1) if n else total for n in range(6)]
    g00, g01, g02, g11, g12, g22 = m[1], m[2], m[3], m[2] + m[3], m[3] + m[4], m[5]
    f1, f2 = g01 / g00, g02 / g00
    a11, a12, h1 = g11 - f1 * g01, g12 - f1 * g02, g00 - f1 * m[0]
    a22, h2 = g22 - f2 * g02, g01 - g00 - f2 * m[0]
    f3 = a12 / a11
    c2 = (h2 - f3 * h1) / (a22 - f3 * a12)
    c1 = (h1 - a12 * c2) / a11
    c0 = (m[0] - g01 * c1 - g02 * c2) / g00
    rd = tile(rd_ref)
    at = iota((K, 128), 0) == iota((K, 128), 1)
    cols = []
    for n, c in enumerate((c0, c1, c2)):
        col = jnp.sum(jnp.where(at, c[0:1], 0.0), axis=1, keepdims=True)
        cols.append(col)
        c_ref[n] = jnp.broadcast_to(col, (K, TC))
    xp = cols[0] * v0p_ref[...] + cols[1] * v1p_ref[...] + cols[2] * v2p_ref[...]
    xp_ref[...] = xp[:, 0:OWN]

    def one(k, carry):
        c0, c1, c2 = (c_ref[n, pl.ds(k, 1), :] for n in range(3))
        xd_ref[k] = (c0 * b_ref[k]) * rd + c1 * v1_ref[k] + c2 * v2_ref[k]
        return carry

    for c in range(CHUNKS):
        lax.fori_loop(4 * c, 4 * c + 4, one, 0)
        mv.flush(0, c)


def f32(*shape):
    return jax.ShapeDtypeStruct(shape, jnp.float32)


def vm(*shape):
    return pltpu.VMEM(shape, jnp.float32)


CHUNKS = 4


class Moves:
    def __init__(self):
        self.ins, self.outs, self.pending = {}, {}, []

    def wait(self, n, chunk=None):
        for c in [chunk] if chunk is not None else range(len(self.ins[n])):
            self.ins[n][c].wait()
            self.ins[n][c] = None

    def flush(self, n, chunk=None):
        for c in [chunk] if chunk is not None else range(len(self.outs[n])):
            self.outs[n][c].start()
            self.pending.append(self.outs[n][c])


def parts(ref, mode):
    if mode == "h":
        return [ref]
    step = ref.shape[0] // CHUNKS
    return [ref.at[step * c : step * (c + 1)] for c in range(CHUNKS)]


def call(kernel, ins, outs, scratch, limit=14, **kw):
    imode, omode = [m for _, m in ins], [m for _, m in outs]
    moved = [jax.ShapeDtypeStruct(x.shape, x.dtype) for x, m in ins + outs if m in "hc"]
    count = sum({"h": 1, "c": CHUNKS}.get(m, 0) for m in imode + omode)

    def wrapped(*refs):
        ni, no, nm = len(ins), len(outs), len(moved)
        hbm, bufs, sems, own = refs[: ni + no], list(refs[ni + no :][:nm]), refs[ni + no + nm], refs[ni + no + nm + 1 :]
        mv, given, sem = Moves(), [], 0
        for n, (ref, mode) in enumerate(zip(hbm, imode + omode)):
            if mode not in "hc":
                given.append(ref)
                continue
            buf = bufs.pop(0)
            given.append(buf)
            copies = []
            for x, y in zip(parts(ref, mode), parts(buf, mode)):
                x, y = (x, y) if n < ni else (y, x)
                copies.append(pltpu.make_async_copy(x, y, sems.at[sem]))
                sem += 1
            (mv.ins if n < ni else mv.outs)[n if n < ni else n - ni] = copies
        for copies in sorted(mv.ins.values(), key=len):
            for c in copies:
                c.start()
        kernel(mv, *given, *own)
        for copies in mv.ins.values():
            assert all(c is None for c in copies)
        for c in mv.pending:
            c.wait()

    space = lambda m: pl.BlockSpec(memory_space=pltpu.VMEM if m == "v" else pltpu.HBM)
    return pl.pallas_call(
        wrapped,
        out_shape=tuple(x if m == "v" else pltpu.HBM(x.shape, x.dtype) for x, m in outs),
        in_specs=[space(m) for m in imode],
        out_specs=tuple(space(m) for m in omode),
        scratch_shapes=[pltpu.VMEM(x.shape, x.dtype) for x in moved]
        + [pltpu.SemaphoreType.DMA((max(count, 1),))] + scratch,
        compiler_params=pltpu.CompilerParams(vmem_limit_bytes=limit << 20),
        name=getattr(kernel, "func", kernel).__name__,
        **kw,
    )(*[x if m == "v" else pltpu.with_memory_space_constraint(x, pltpu.HBM) for x, m in ins])


def swapped(x, axes):
    return lax.all_to_all(x, axes, 0, 0, tiled=True)


def body(
    die_current, die_shunt, pkg_current, pkg_matrix, pkg_block_inv, bump_node, bump_conductance
):
    nodes = bump_node.reshape(NB // 128, 128)
    cond = bump_conductance.reshape(NB // 128, 128)
    b, sh, bp, m = die_current, die_shunt, pkg_current, pkg_block_inv
    gathered, small, ext, die = f32(128, 8, 128), f32(K, 128), f32(K, ER, EC), f32(K, TR, TC)
    lattice = f32(6 * K, 128)
    payload = [vm(128 // SENDS, 8, 128), pltpu.SemaphoreType.DMA((SENDS,))]
    alone = [vm(128 // SENDS, 4, 128)] + payload[1:]
    msg1, edge = call(
        load_kernel,
        [(b, "c"), (sh, "h"), (pkg_matrix.reshape(8, OWN, 512), "h")],
        [(f32(8, 128 + HROWS, 128), "r"), (f32(PLANES, 16, TC), "h")],
        [vm(128, 128), pltpu.SemaphoreType.DMA((6,))],
    )
    g1 = swapped(msg1, COL)
    msg, cm, v0p, bump1 = call(
        start_kernel,
        [(b, "h"), (sh, "h"), (bp, "h"), (m, "h"), (nodes, "h"), (cond, "h")],
        [(gathered, "r"), (f32(ER, EC), "h"), (small, "h"), (f32(K + 8, 128), "h")],
        [vm(24, 128), vm(K, 4 * TC), vm(K + 8, 4 * TC), vm(6, TR, TC), vm(K, 128)] + payload,
    )
    g = swapped(msg, ROW_COL)
    side, up, dn = call(
        columns_kernel,
        [(g1, "v"), (edge, "h")],
        [(f32(PLANES, TR, 128), "v"), (f32(PAIRS, 8, EC), "v"), (f32(PAIRS, 8, EC), "v")],
        [vm(128, 128), vm(2, PLANES, 8, EC)],
    )
    n = lax.axis_size(ROW)
    bot = lax.ppermute(up, ROW, [(r + 1, r) for r in range(n - 1)])
    top = lax.ppermute(dn, ROW, [(r, r + 1) for r in range(n - 1)])
    side, grp, bump1, pm = call(
        edges_kernel,
        [(sh, "h"), (side, "v"), (bot, "v"), (top, "v"), (cm, "h"), (g1, "v"), (bump1, "h")],
        [
            (f32(PLANES, TR, 128), "r"), (f32(PLANES, 8, EC), "h"), (f32(K + 8, 128), "h"),
            (f32(OWN, NB), "h"),
        ],
        [vm(K, 4 * TC), vm(K, 512), pltpu.SemaphoreType.DMA((1,))],
    )
    step = [vm(K, NB), vm(K, 128)]
    results = [(small, "h"), (small, "h"), (small, "h"), (lattice, "h")]
    v1p, _, y1, near, msg = call(
        functools.partial(package_kernel, 1),
        [(g, "v"), (pm, "h"), (m, "h"), (cond, "h"), (bump1, "h"), (bump1, "h"), (v0p, "h")],
        results + [(gathered, "r")],
        step + payload,
    )
    g = swapped(msg, ROW_COL)
    v1, bump2, r, rd, dg, cr, near1 = call(
        second_kernel,
        [(b, "c")] + [(x, "h") for x in (sh, side, grp, cm, near, bp, v0p, v1p, y1)],
        [
            (die, "c"), (small, "v"), (f32(3 * K, 128), "h"), (f32(ER, EC), "h"),
            (f32(TR, TC), "h"), (f32(ER, EC), "h"), (ext, "c"),
        ],
        [vm(6 * K, EC), vm(K, 4 * TC), vm(K, 128), vm(ER, EC)],
    )
    wp, wd, y2, near, msg = call(
        functools.partial(package_kernel, 2),
        [(g, "v"), (pm, "h"), (m, "h"), (cond, "h"), (bump2, "v"), (bump1, "h"), (v1p, "h")],
        results + [(f32(128, 4, 128), "r")],
        step + alone,
    )
    g = swapped(msg, ROW_COL)
    w, r = call(
        third_kernel,
        [(near1, "c"), (v1, "c")] + [(x, "h") for x in (rd, dg, cr, near, wp, y1, y2, r)],
        [(die, "c"), (f32(128, 128), "v")],
        [vm(6 * K, EC)],
    )
    msg, v1, w = call(
        fourth_kernel,
        [(g, "v")] + [(x, "h") for x in (pm, cond, bump1, wp, wd)] + [(r, "v"), (v1, "r"), (w, "r")],
        [(f32(128, 1, 128), "v"), (die, "v"), (die, "v")],
        [vm(K, NB), vm(K, 128), vm(128, 128), pltpu.SemaphoreType.DMA((2,))],
    )
    g = swapped(msg, ROW_COL)
    return call(
        last_kernel,
        [(x, "v") for x in (g, b, rd, v1, w, v0p, v1p, wp)],
        [(die, "c"), (f32(K, OWN), "v")],
        [vm(3, K, TC)],
    )


def solution(mesh):
    torus = Mesh(mesh.devices.reshape(2, 4, 2, 4, 2), ROW_COL)
    placed = (
        P(None, ROW, COL),
        P(ROW, COL),
        P(None, ROW_COL),
        P(ROW, COL),
        P(ROW_COL, None, None),
        P(),
        P(),
    )
    return jax.shard_map(
        body,
        mesh=torus,
        in_specs=placed,
        out_specs=(P(None, ROW, COL), P(None, ROW_COL)),
        check_vma=False,
    )
```

```python
import functools

import jax
import jax.numpy as jnp
from jax import lax
from jax.experimental import pallas as pl
from jax.experimental.pallas import tpu as pltpu
from jax.sharding import Mesh
from jax.sharding import PartitionSpec as P

ROW = ("row_0", "row_1", "row_2")
COL = ("col_0", "col_1")
ROW_COL = ("row_0", "row_1", "row_2", "col_0", "col_1")

K = 16
TR, TC = 128, 256
ER, EC = 136, 384
CELL = 32
PLANES = K + 1
PAIRS = 9
HROWS = 56
OWN = 32
NB = 4096
HI = lax.Precision.HIGHEST


def iota(shape, dim):
    return lax.broadcasted_iota(jnp.int32, shape, dim)


def where_am_i():
    i = (lax.axis_index("row_0") * 4 + lax.axis_index("row_1")) * 2 + lax.axis_index("row_2")
    j = lax.axis_index("col_0") * 2 + lax.axis_index("col_1")
    return i, j


def dot_nt(a, b):
    return lax.dot_general(
        a, b, (((1,), (1,)), ((), ())), precision=HI, preferred_element_type=jnp.float32
    )


def dot_nn(a, b):
    return jnp.dot(a, b, precision=HI, preferred_element_type=jnp.float32)


def spread(j):
    group = iota((128, EC), 1) // CELL
    cell = jnp.where(group <= 8, 8 * j + group, jnp.where(group == 11, 8 * j - 1, -5))
    return (iota((128, EC), 0) % 64 == cell).astype(jnp.float32)


def lattice_chunk(l):
    return jnp.clip(l // 2, 0, NB // 128 - 1)


def extended_rows(parts):
    body = [jnp.broadcast_to(p, (CELL, EC)) for p in parts[1:5]]
    edge = jnp.where(iota((8, EC), 0) < 4, parts[5], parts[0])
    return jnp.concatenate(body + [edge], axis=0)


def padded(scr, x):
    scr[...] = jnp.zeros_like(scr)
    scr[:, 0 : x.shape[1]] = x
    return scr[...]


def pack(vp, vd):
    lane = iota((8, 128), 1)
    hi = pltpu.roll(vp[8:16], 32, 1)
    out = jnp.where(lane < 32, vp[0:8], hi)
    out = jnp.where(lane < 64, out, pltpu.roll(vd[0:8], 64, 1))
    return jnp.where(lane < 96, out, pltpu.roll(vd[8:16], 96, 1))


def pack_package(vp):
    lane = iota((4, 128), 1)
    out = vp[0:4]
    for m in range(1, 4):
        out = jnp.where(lane // 32 == m, pltpu.roll(vp, 32 * m, 1)[4 * m : 4 * m + 4], out)
    return out


def gather_bumps(s_ref):
    at = iota((4 * TC, 128), 0)
    pick = (at // TC * 8 + at % TC // CELL == iota((4 * TC, 128), 1)).astype(jnp.float32)
    return dot_nn(s_ref[...], pick)


def down_cells(s_ref, k, z):
    for lr in range(4):
        rows = z[CELL * lr : CELL * (lr + 1)]
        s_ref[pl.ds(k, 1), TC * lr : TC * (lr + 1)] = jnp.sum(rows, axis=0, keepdims=True)


SENDS = 8


def send(msg_hbm, pay_ref, sems, pay):
    n = pay_ref.shape[0]
    for d in range(n):
        pay_ref[d] = pay
    copies = [
        pltpu.make_async_copy(pay_ref, msg_hbm.at[n * c : n * (c + 1)], sems.at[c]) for c in range(SENDS)
    ]
    for c in copies:
        c.start()
    return copies


def load_kernel(mv, b_ref, sh_ref, p_ref, msg_hbm, edge_ref, z_ref, sems):
    _, j = where_am_i()
    mv.wait(2)
    rows = [
        pltpu.make_async_copy(
            p_ref.at[:, :, 128 * t : 128 * (t + 1)],
            msg_hbm.at[:, 32 * t : 32 * (t + 1), :],
            sems.at[t],
        )
        for t in range(4)
    ]
    for c in rows:
        c.start()
    lane = iota((TR, 128), 1)
    z = jnp.zeros((TR, 128), jnp.float32)
    mv.wait(1)
    for k in [K] + list(range(K)):
        if k < K and k % 4 == 0:
            mv.wait(0, k // 4)
        src = b_ref.at[k] if k < K else sh_ref
        lo = pltpu.roll(src[:, 0:128], 3 * k, 1) if k else src[:, 0:128]
        up = pltpu.roll(src[:, 128:256], (64 + 3 * k - 125) % 128, 1)
        z = jnp.where((lane >= 3 * k) & (lane < 3 * k + 3), lo, z)
        z = jnp.where((lane >= 64 + 3 * k) & (lane < 67 + 3 * k), up, z)
        edge_ref[k, 0:8, :] = src[0:8, :]
        edge_ref[k, 8:16, :] = src[TR - 8 : TR, :]
    mv.flush(1)
    z_ref[...] = z.T
    side = lambda at, to, n: pltpu.make_async_copy(
        z_ref.at[at : at + HROWS, :], msg_hbm.at[to, 128 : 128 + HROWS, :], sems.at[n]
    )
    sides = [side(0, jnp.maximum(j - 1, 0), 4), side(64, jnp.minimum(j + 1, 7), 5)]
    for c in sides:
        c.start()
    for c in sides + rows:
        c.wait()


def start_kernel(
    mv, b_ref, sh_ref, bp_ref, m_ref, node_ref, cond_ref,
    msg_hbm, cm_ref, v0p_ref, bump_ref,
    a_ref, s_ref, t_ref, w_ref, pad_ref, pay_ref, sems,
):
    i, j = where_am_i()
    for n in (4, 5):
        mv.wait(n)
    a_ref[...] = jnp.zeros_like(a_ref)
    ln = iota((1, 128), 1)
    for lr in range(6):
        l = 4 * i + lr - 1
        chunk = lattice_chunk(l)
        ok = (ln // 64 == l % 2) & (l >= 0) & (l < 64)
        nd = node_ref[pl.ds(chunk, 1), :]
        a_ref[lr : lr + 1, :] = jnp.where(ok, nd // 2048 - CELL * l, 0).astype(jnp.float32)
        a_ref[8 + lr : 9 + lr, :] = jnp.where(ok, nd % 2048 - CELL * (ln % 64), 0).astype(jnp.float32)
        a_ref[16 + lr : 17 + lr, :] = jnp.where(ok, cond_ref[pl.ds(chunk, 1), :], 0.0)
    wide = dot_nn(a_ref[...], spread(j))
    maps = [extended_rows([wide[8 * n + lr : 8 * n + lr + 1] for lr in range(6)]) for n in range(3)]
    row = iota((ER, EC), 0)
    here = jnp.where(row < TR, row % CELL, jnp.where(row < TR + 4, row - TR, row - TR + 24))
    cols = iota((ER, EC), 1) % CELL
    hit = (maps[0].astype(jnp.int32) == here) & (maps[1].astype(jnp.int32) == cols)
    cm = jnp.where(hit, maps[2], 0.0)
    cm_ref[...] = cm
    mv.flush(1)
    mv.wait(1)
    here = cm[0:TR, 0:TC]
    rd = 1.0 / (4.0 + sh_ref[...] + here)
    at_bump = jnp.where(here > 0.0, rd, 0.0)
    row, col = iota((TR, TC), 0), iota((TR, TC), 1)
    w_ref[0] = rd
    w_ref[1] = at_bump
    for n, inside in enumerate((row > 0, row < TR - 1, col > 0, col < TC - 1)):
        w_ref[2 + n] = jnp.where(inside, at_bump, 0.0)

    def one(k, c):
        x = b_ref[k] * w_ref[0]
        at = b_ref[k] * w_ref[1]
        down_cells(s_ref, k, at)
        near = pltpu.roll(x, 1, 0) * w_ref[2] + pltpu.roll(x, TR - 1, 0) * w_ref[3]
        near = near + pltpu.roll(x, 1, 1) * w_ref[4] + pltpu.roll(x, TC - 1, 1) * w_ref[5]
        down_cells(t_ref, k, at - near)
        return c

    mv.wait(0)
    lax.fori_loop(0, K, one, 0)
    t_ref[K : K + 8, :] = jnp.zeros((8, 4 * TC), jnp.float32)
    down_cells(t_ref, K, here)
    down_cells(t_ref, K + 1, here * rd)
    bump_ref[...] = gather_bumps(t_ref)
    mv.flush(3)
    mv.wait(2)
    mv.wait(3)
    v0p = padded(pad_ref, dot_nt(bp_ref[...], m_ref[0]))
    v0p_ref[...] = v0p
    mv.flush(2)
    for c in send(msg_hbm, pay_ref, sems, pack(v0p, gather_bumps(s_ref))):
        c.wait()


def columns_kernel(mv, g1_ref, edge_ref, w_ref, up_ref, dn_ref, y_ref, ext_ref):
    _, j = where_am_i()
    y_ref[...] = jnp.zeros_like(y_ref)

    @pl.when(j < 7)
    def _():
        y_ref[0:HROWS, :] = g1_ref[jnp.minimum(j + 1, 7), 128 : 128 + HROWS, :]

    @pl.when(j > 0)
    def _():
        y_ref[64 : 64 + HROWS, :] = g1_ref[jnp.maximum(j - 1, 0), 128 : 128 + HROWS, :]

    yt = y_ref[...].T
    lane = iota((TR, 128), 1)
    for k in range(PLANES):
        right = pltpu.roll(yt, (128 - 3 * k) % 128, 1) if k else yt
        left = pltpu.roll(yt, (61 - 3 * k) % 128, 1) if (61 - 3 * k) % 128 else yt
        w_ref[k] = jnp.where(lane < 3, right, jnp.where(lane >= 125, left, 0.0))
    first = iota((8, EC), 0) < 4
    mv.wait(1)
    for k in range(PLANES):
        for side in range(2):
            ext_ref[side, k, :, 0:TC] = edge_ref[k, 8 * side : 8 * side + 8, :]
            ext_ref[side, k, :, TC:EC] = w_ref[k, (TR - 8) * side : (TR - 8) * side + 8, :]
    for p in range(PAIRS):
        q = min(p + PAIRS, PLANES - 1)
        up_ref[p] = jnp.where(first, ext_ref[0, p], pltpu.roll(ext_ref[0, q], 4, 0))
        dn_ref[p] = jnp.where(first, pltpu.roll(ext_ref[1, p], 4, 0), ext_ref[1, q])


def whole_plane(xs_ref, main, w_ref, grp_ref, k):
    xs_ref[0:TR, 0:TC] = main
    xs_ref[0:TR, TC:EC] = w_ref[k]
    xs_ref[TR:ER, :] = grp_ref[k]
    return xs_ref[...]


def package_all(g_ref, v_ref):
    lane = iota((8, 128), 1) // 32

    def one(c, carry):
        lo = jnp.zeros((8, 128), jnp.float32)
        hi = jnp.zeros((8, 128), jnp.float32)
        for m in range(4):
            x = g_ref[4 * c + m]
            lo = jnp.where(lane == m, pltpu.roll(x, 32 * m, 1) if m else x, lo)
            hi = jnp.where(lane == m, pltpu.roll(x, (32 * m - 32) % 128, 1) if m != 1 else x, hi)
        at = pl.ds(pl.multiple_of(128 * c, 128), 128)
        v_ref[0:8, at] = lo
        v_ref[8:16, at] = hi
        return carry

    lax.fori_loop(0, NB // 128, one, 0, unroll=4)


def package_only(g_ref, v_ref):
    lane = iota((4, 128), 1) // 32

    def one(c, carry):
        xs = [g_ref[4 * c + d] for d in range(4)]
        at = pl.ds(pl.multiple_of(128 * c, 128), 128)
        for m in range(4):
            out = xs[m]
            for d in range(4):
                if d != m:
                    out = jnp.where(lane == d, pltpu.roll(xs[d], (32 * (d - m)) % 128, 1), out)
            v_ref[4 * m : 4 * m + 4, at] = out
        return carry

    lax.fori_loop(0, NB // 128, one, 0, unroll=4)


def own_die(g_ref, i, j):
    lane = iota((8, 128), 1)
    halves = []
    for h in range(2):
        out = jnp.zeros((8, 128), jnp.float32)
        for m in range(4):
            x = g_ref[8 * i + 4 * (j % 2) + m]
            shift = 8 * m - (64 + 32 * h + 8 * (j // 2)) + 128
            x = pltpu.roll(x, shift % 128, 1)
            out = jnp.where((lane >= 8 * m) & (lane < 8 * m + 8), x, out)
        halves.append(out)
    return jnp.concatenate(halves, axis=0)


def own_conductance(cond_ref, i, j):
    q = 8 * i + j
    row = cond_ref[pl.ds(q // 4, 1), :]
    return pltpu.roll(row, (128 - 32 * (q % 4)) % 128, 1)


def around(v_ref, x_ref, i):
    ln = iota((K, 128), 1)
    for lr in range(6):
        l = 4 * i + lr - 1
        at = pl.ds(pl.multiple_of(128 * lattice_chunk(l), 128), 128)
        x_ref[K * lr : K * (lr + 1), :] = jnp.where(ln // 64 == l % 2, v_ref[:, at], 0.0)


def coupled(e_ref, k):
    return extended_rows([e_ref[pl.ds(K * lr + k, 1), :] for lr in range(6)])


def beside(x):
    out = pltpu.roll(x, 1, 0) + pltpu.roll(x, ER - 1, 0)
    return out + pltpu.roll(x, 1, 1) + pltpu.roll(x, EC - 1, 1)


def add_dot(r_ref, at, x):
    s = jnp.sum(x, axis=0, keepdims=True)
    r_ref[pl.ds(at, 1), :] = s[:, 0:128] + s[:, 128:256]


def tile(x):
    return x[0:TR, 0:TC]


def edges_kernel(
    mv, sh_ref, w_ref, bot_ref, top_ref, cm_ref, g1_ref, inner_ref,
    w_hbm, grp_ref, bump_ref, pm_ref,
    s_ref, t_ref, sem,
):
    keep = pltpu.make_async_copy(w_ref, w_hbm, sem.at[0])
    keep.start()
    for d in range(8):
        for t in range(4):
            c = 4 * d + t
            pm_ref[:, 128 * c : 128 * (c + 1)] = g1_ref[d, 32 * t : 32 * (t + 1), :]
    first = iota((8, EC), 0) < 4
    for p in range(PAIRS):
        bot, top = bot_ref[p], top_ref[p]
        grp_ref[p] = jnp.where(first, bot, pltpu.roll(top, 4, 0))
        if p + PAIRS < PLANES:
            grp_ref[p + PAIRS] = jnp.where(first, pltpu.roll(bot, 4, 0), top)
    mv.flush(1)
    for n in (0, 4, 6):
        mv.wait(n)
    inverse = lambda sh, cm: jnp.where(sh > 0.0, 1.0 / (4.0 + sh + cm), 0.0)
    cm = tile(cm_ref)
    at_bump = jnp.where(cm > 0.0, inverse(sh_ref[...], cm), 0.0)
    ends = inverse(grp_ref[K], cm_ref[TR:ER, :])
    above = ends[7:8, 0:TC] * at_bump[0:1]
    below = ends[0:1, 0:TC] * at_bump[TR - 1 : TR]
    lane = iota((TR, 128), 1)
    sides = jnp.where(lane == 0, pltpu.roll(at_bump[:, 128:256], 1, 1), 0.0)
    sides = jnp.where(lane == 127, pltpu.roll(at_bump[:, 0:128], 127, 1), sides)
    sides = sides * inverse(w_ref[K], cm_ref[0:TR, TC:EC])
    s_ref[...] = jnp.zeros_like(s_ref)
    for k in range(K):
        s_ref[k : k + 1, 0:TC] = grp_ref[k, 7:8, 0:TC] * above
        s_ref[k : k + 1, 3 * TC : 4 * TC] = grp_ref[k, 0:1, 0:TC] * below
        z = w_ref[k] * sides
        for lr in range(4):
            t_ref[k : k + 1, 128 * lr : 128 * (lr + 1)] = jnp.sum(
                z[CELL * lr : CELL * (lr + 1)], axis=0, keepdims=True
            )
    at, to = iota((512, 128), 0), iota((512, 128), 1)
    right = (at % 128 == 0) & (to == at // 128 * 8 + 7)
    left = (at % 128 == 127) & (to == at // 128 * 8)
    halo = gather_bumps(s_ref) + dot_nn(t_ref[...], (left | right).astype(jnp.float32))
    bump_ref[0:K, :] = inner_ref[0:K, :] - halo
    bump_ref[K:, :] = inner_ref[K:, :]
    mv.flush(2)
    keep.wait()


def package_kernel(
    step, mv, g_ref, pm_ref, m_ref, cond_ref, bump_ref, const_ref, vp_ref,
    out_ref, vd_ref, y_ref, x_ref, msg_hbm,
    v_ref, pad_ref, pay_ref, sems,
):
    i, j = where_am_i()
    package_all(g_ref, v_ref)
    for n in range(1, 7):
        if n in mv.ins:
            mv.wait(n)
    vp = vp_ref[...]
    y = padded(pad_ref, dot_nt(v_ref[...], pm_ref[...]))
    y = y + own_conductance(cond_ref, i, j) * (vp - own_die(g_ref, i, j))
    y = jnp.where(iota((K, 128), 1) < OWN, y, 0.0)
    out = padded(pad_ref, dot_nt(y[:, 0:OWN], m_ref[0]))
    if step == 2:
        out = out - vp
    vd = bump_ref[0:K, :] - const_ref[K + 1 : K + 2, :] * at_tile(v_ref, i, j)
    sent = send(msg_hbm, pay_ref, sems, pack(out, vd) if step == 1 else pack_package(out))
    y_ref[...] = y
    out_ref[...] = out
    vd_ref[...] = vd
    around(v_ref, x_ref, i)
    for n in range(4):
        mv.flush(n)
    for c in sent:
        c.wait()


def at_tile(v_ref, i, j):
    ln = iota((K, 128), 1)
    out = jnp.zeros((K, 128), jnp.float32)
    for lr in range(4):
        l = 4 * i + lr
        at = pl.ds(pl.multiple_of(128 * lattice_chunk(l), 128), 128)
        x = pltpu.roll(v_ref[:, at], (8 * lr - 64 * (l % 2) - 8 * j + 256) % 128, 1)
        out = jnp.where((ln >= 8 * lr) & (ln < 8 * lr + 8), x, out)
    return out


def second_kernel(
    mv, b_ref, sh_ref, w_ref, grp_ref, cm_ref, x_ref, bp_ref, v0p_ref, v1p_ref, y1_ref,
    v1_ref, bump_ref, r_ref, rd_ref, dg_ref, cr_ref, next_ref,
    e_ref, s_ref, pad_ref, xs_ref,
):
    i, j = where_am_i()
    for n in range(1, 10):
        mv.wait(n)
    sh = whole_plane(xs_ref, sh_ref[...], w_ref, grp_ref, K)
    cm = cm_ref[...]
    rd = jnp.where(sh > 0.0, 1.0 / (4.0 + sh + cm), 0.0)
    rd_ref[...] = rd
    cr_ref[...] = cm * rd
    dg_ref[...] = 4.0 + tile(sh) + tile(cm)
    for n in (3, 4, 5):
        mv.flush(n)
    e_ref[...] = dot_nn(x_ref[...], spread(j))

    def one(k, c):
        rd, dg = rd_ref[...], dg_ref[...]
        x0 = whole_plane(xs_ref, b_ref[k], w_ref, grp_ref, k) * rd
        x1 = x0 - (beside(x0) * rd + cr_ref[...] * coupled(e_ref, k))
        v1_ref[k] = tile(x1)
        near = -beside(x1) * rd
        next_ref[k] = near
        down_cells(s_ref, k, jnp.where(tile(cr_ref) > 0.0, tile(near), 0.0))
        a, b = tile(x0), tile(x1)
        add_dot(r_ref, k, dg * a * a)
        add_dot(r_ref, K + k, dg * a * b)
        add_dot(r_ref, 2 * K + k, dg * b * b)
        return c

    for c in range(CHUNKS):
        mv.wait(0, c)
        lax.fori_loop(4 * c, 4 * c + 4, one, 0)
        mv.flush(0, c)
        mv.flush(6, c)
    bump_ref[...] = gather_bumps(s_ref)
    v0p, v1p, y1 = v0p_ref[...], v1p_ref[...], y1_ref[...]
    bp = padded(pad_ref, bp_ref[...])
    r_ref[0:K, :] += v0p * bp
    r_ref[K : 2 * K, :] += v0p * y1
    r_ref[2 * K : 3 * K, :] += v1p * y1
    mv.flush(2)


def third_kernel(
    mv, next_ref, v1_ref, rd_ref, dg_ref, cr_ref, x_ref, wp_ref, y1_ref, y2_ref, ra_ref,
    wt_ref, r_ref,
    e_ref,
):
    i, j = where_am_i()
    for n in range(2, 10):
        mv.wait(n)
    e_ref[...] = dot_nn(x_ref[...], spread(j))
    r_ref[6 * K :, :] = jnp.zeros((2 * K, 128), jnp.float32)
    r_ref[0 : 3 * K, :] = ra_ref[...]

    def one(k, c):
        dg = dg_ref[...]
        w = next_ref[k] - cr_ref[...] * coupled(e_ref, k)
        a, b = v1_ref[k], tile(w)
        wt_ref[k] = b
        add_dot(r_ref, 3 * K + k, dg * a * b)
        add_dot(r_ref, 4 * K + k, dg * b * b)
        add_dot(r_ref, 5 * K + k, dg * b * (b - tile(beside(w)) * tile(rd_ref)))
        return c

    for c in range(CHUNKS):
        mv.wait(0, c)
        mv.wait(1, c)
        lax.fori_loop(4 * c, 4 * c + 4, one, 0)
        mv.flush(0, c)
    wp, y1, y2 = wp_ref[...], y1_ref[...], y2_ref[...]
    r_ref[3 * K : 4 * K, :] += wp * y1
    r_ref[4 * K : 5 * K, :] += wp * (y2 - y1)


def fourth_kernel(
    mv, g_ref, pm_ref, cond_ref, const_ref, wp_ref, wd_ref, ra_ref, v1_hbm, w_hbm,
    msg_ref, v1_ref, w_ref,
    v_ref, pad_ref, r_ref, sems,
):
    i, j = where_am_i()
    loads = [
        pltpu.make_async_copy(v1_hbm, v1_ref, sems.at[0]),
        pltpu.make_async_copy(w_hbm, w_ref, sems.at[1]),
    ]
    for c in loads:
        c.start()
    package_only(g_ref, v_ref)
    for n in range(2, 6):
        mv.wait(n)
    wp = wp_ref[...]
    y = padded(pad_ref, dot_nt(v_ref[...], pm_ref[...])) + own_conductance(cond_ref, i, j) * wp
    y = jnp.where(iota((K, 128), 1) < OWN, y, 0.0)
    r_ref[...] = ra_ref[...]
    both = const_ref[K : K + 1, :] * wd_ref[...] * at_tile(v_ref, i, j)
    r_ref[5 * K : 6 * K, :] += wp * y - 2.0 * both
    sums = dot_nt(jnp.ones((8, 128), jnp.float32), r_ref[...])

    def one(d, c):
        msg_ref[d] = sums[0:1]
        return c

    lax.fori_loop(0, msg_ref.shape[0], one, 0, unroll=8)
    for c in loads:
        c.wait()


def last_kernel(
    mv, g_ref, b_ref, rd_ref, v1_ref, v2_ref, v0p_ref, v1p_ref, v2p_ref,
    xd_ref, xp_ref, c_ref,
):
    total = jnp.sum(g_ref[...], axis=0)
    total = jnp.broadcast_to(total, (8, 128))
    m = [pltpu.roll(total, (128 - K * n) % 128, 1) if n else total for n in range(6)]
    g00, g01, g02, g11, g12, g22 = m[1], m[2], m[3], m[2] + m[3], m[3] + m[4], m[5]
    f1, f2 = g01 / g00, g02 / g00
    a11, a12, h1 = g11 - f1 * g01, g12 - f1 * g02, g00 - f1 * m[0]
    a22, h2 = g22 - f2 * g02, g01 - g00 - f2 * m[0]
    f3 = a12 / a11
    c2 = (h2 - f3 * h1) / (a22 - f3 * a12)
    c1 = (h1 - a12 * c2) / a11
    c0 = (m[0] - g01 * c1 - g02 * c2) / g00
    rd = tile(rd_ref)
    at = iota((K, 128), 0) == iota((K, 128), 1)
    cols = []
    for n, c in enumerate((c0, c1, c2)):
        col = jnp.sum(jnp.where(at, c[0:1], 0.0), axis=1, keepdims=True)
        cols.append(col)
        c_ref[n] = jnp.broadcast_to(col, (K, TC))
    xp = cols[0] * v0p_ref[...] + cols[1] * v1p_ref[...] + cols[2] * v2p_ref[...]
    xp_ref[...] = xp[:, 0:OWN]

    def one(k, carry):
        c0, c1, c2 = (c_ref[n, pl.ds(k, 1), :] for n in range(3))
        xd_ref[k] = (c0 * b_ref[k]) * rd + c1 * v1_ref[k] + c2 * v2_ref[k]
        return carry

    for c in range(CHUNKS):
        lax.fori_loop(4 * c, 4 * c + 4, one, 0)
        mv.flush(0, c)


def f32(*shape):
    return jax.ShapeDtypeStruct(shape, jnp.float32)


def vm(*shape):
    return pltpu.VMEM(shape, jnp.float32)


CHUNKS = 4


class Moves:
    def __init__(self):
        self.ins, self.outs, self.pending = {}, {}, []

    def wait(self, n, chunk=None):
        for c in [chunk] if chunk is not None else range(len(self.ins[n])):
            self.ins[n][c].wait()
            self.ins[n][c] = None

    def flush(self, n, chunk=None):
        for c in [chunk] if chunk is not None else range(len(self.outs[n])):
            self.outs[n][c].start()
            self.pending.append(self.outs[n][c])


def parts(ref, mode):
    if mode == "h":
        return [ref]
    step = ref.shape[0] // CHUNKS
    return [ref.at[step * c : step * (c + 1)] for c in range(CHUNKS)]


def call(kernel, ins, outs, scratch, limit=14, **kw):
    imode, omode = [m for _, m in ins], [m for _, m in outs]
    moved = [jax.ShapeDtypeStruct(x.shape, x.dtype) for x, m in ins + outs if m in "hc"]
    count = sum({"h": 1, "c": CHUNKS}.get(m, 0) for m in imode + omode)

    def wrapped(*refs):
        ni, no, nm = len(ins), len(outs), len(moved)
        hbm, bufs, sems, own = refs[: ni + no], list(refs[ni + no :][:nm]), refs[ni + no + nm], refs[ni + no + nm + 1 :]
        mv, given, sem = Moves(), [], 0
        for n, (ref, mode) in enumerate(zip(hbm, imode + omode)):
            if mode not in "hc":
                given.append(ref)
                continue
            buf = bufs.pop(0)
            given.append(buf)
            copies = []
            for x, y in zip(parts(ref, mode), parts(buf, mode)):
                x, y = (x, y) if n < ni else (y, x)
                copies.append(pltpu.make_async_copy(x, y, sems.at[sem]))
                sem += 1
            (mv.ins if n < ni else mv.outs)[n if n < ni else n - ni] = copies
        for copies in sorted(mv.ins.values(), key=len):
            for c in copies:
                c.start()
        kernel(mv, *given, *own)
        for copies in mv.ins.values():
            assert all(c is None for c in copies)
        for c in mv.pending:
            c.wait()

    space = lambda m: pl.BlockSpec(memory_space=pltpu.VMEM if m == "v" else pltpu.HBM)
    return pl.pallas_call(
        wrapped,
        out_shape=tuple(x if m == "v" else pltpu.HBM(x.shape, x.dtype) for x, m in outs),
        in_specs=[space(m) for m in imode],
        out_specs=tuple(space(m) for m in omode),
        scratch_shapes=[pltpu.VMEM(x.shape, x.dtype) for x in moved]
        + [pltpu.SemaphoreType.DMA((max(count, 1),))] + scratch,
        compiler_params=pltpu.CompilerParams(vmem_limit_bytes=limit << 20),
        name=getattr(kernel, "func", kernel).__name__,
        **kw,
    )(*[x if m == "v" else pltpu.with_memory_space_constraint(x, pltpu.HBM) for x, m in ins])


def swapped(x, axes):
    return lax.all_to_all(x, axes, 0, 0, tiled=True)


def body(
    die_current, die_shunt, pkg_current, pkg_matrix, pkg_block_inv, bump_node, bump_conductance
):
    nodes = bump_node.reshape(NB // 128, 128)
    cond = bump_conductance.reshape(NB // 128, 128)
    b, sh, bp, m = die_current, die_shunt, pkg_current, pkg_block_inv
    gathered, small, ext, die = f32(128, 8, 128), f32(K, 128), f32(K, ER, EC), f32(K, TR, TC)
    lattice = f32(6 * K, 128)
    payload = [vm(128 // SENDS, 8, 128), pltpu.SemaphoreType.DMA((SENDS,))]
    alone = [vm(128 // SENDS, 4, 128)] + payload[1:]
    msg1, edge = call(
        load_kernel,
        [(b, "c"), (sh, "h"), (pkg_matrix.reshape(8, OWN, 512), "h")],
        [(f32(8, 128 + HROWS, 128), "r"), (f32(PLANES, 16, TC), "h")],
        [vm(128, 128), pltpu.SemaphoreType.DMA((6,))],
    )
    g1 = swapped(msg1, COL)
    msg, cm, v0p, bump1 = call(
        start_kernel,
        [(b, "h"), (sh, "h"), (bp, "h"), (m, "h"), (nodes, "h"), (cond, "h")],
        [(gathered, "r"), (f32(ER, EC), "h"), (small, "h"), (f32(K + 8, 128), "h")],
        [vm(24, 128), vm(K, 4 * TC), vm(K + 8, 4 * TC), vm(6, TR, TC), vm(K, 128)] + payload,
    )
    g = swapped(msg, ROW_COL)
    side, up, dn = call(
        columns_kernel,
        [(g1, "v"), (edge, "h")],
        [(f32(PLANES, TR, 128), "v"), (f32(PAIRS, 8, EC), "v"), (f32(PAIRS, 8, EC), "v")],
        [vm(128, 128), vm(2, PLANES, 8, EC)],
    )
    n = lax.axis_size(ROW)
    bot = lax.ppermute(up, ROW, [(r + 1, r) for r in range(n - 1)])
    top = lax.ppermute(dn, ROW, [(r, r + 1) for r in range(n - 1)])
    side, grp, bump1, pm = call(
        edges_kernel,
        [(sh, "h"), (side, "v"), (bot, "v"), (top, "v"), (cm, "h"), (g1, "v"), (bump1, "h")],
        [
            (f32(PLANES, TR, 128), "r"), (f32(PLANES, 8, EC), "h"), (f32(K + 8, 128), "h"),
            (f32(OWN, NB), "v"),
        ],
        [vm(K, 4 * TC), vm(K, 512), pltpu.SemaphoreType.DMA((1,))],
    )
    step = [vm(K, NB), vm(K, 128)]
    results = [(small, "h"), (small, "h"), (small, "h"), (lattice, "h")]
    v1p, _, y1, near, msg = call(
        functools.partial(package_kernel, 1),
        [(g, "v"), (pm, "v"), (m, "h"), (cond, "h"), (bump1, "h"), (bump1, "h"), (v0p, "h")],
        results + [(gathered, "r")],
        step + payload,
    )
    g = swapped(msg, ROW_COL)
    v1, bump2, r, rd, dg, cr, near1 = call(
        second_kernel,
        [(b, "c")] + [(x, "h") for x in (sh, side, grp, cm, near, bp, v0p, v1p, y1)],
        [
            (die, "c"), (small, "v"), (f32(3 * K, 128), "h"), (f32(ER, EC), "h"),
            (f32(TR, TC), "h"), (f32(ER, EC), "h"), (ext, "c"),
        ],
        [vm(6 * K, EC), vm(K, 4 * TC), vm(K, 128), vm(ER, EC)],
    )
    wp, wd, y2, near, msg = call(
        functools.partial(package_kernel, 2),
        [(g, "v"), (pm, "v"), (m, "h"), (cond, "h"), (bump2, "v"), (bump1, "h"), (v1p, "h")],
        results + [(f32(128, 4, 128), "r")],
        step + alone,
    )
    g = swapped(msg, ROW_COL)
    w, r = call(
        third_kernel,
        [(near1, "c"), (v1, "c")] + [(x, "h") for x in (rd, dg, cr, near, wp, y1, y2, r)],
        [(die, "c"), (f32(128, 128), "v")],
        [vm(6 * K, EC)],
    )
    msg, v1, w = call(
        fourth_kernel,
        [(g, "v"), (pm, "v")] + [(x, "h") for x in (cond, bump1, wp, wd)] + [(r, "v"), (v1, "r"), (w, "r")],
        [(f32(128, 1, 128), "v"), (die, "v"), (die, "v")],
        [vm(K, NB), vm(K, 128), vm(128, 128), pltpu.SemaphoreType.DMA((2,))],
    )
    g = swapped(msg, ROW_COL)
    return call(
        last_kernel,
        [(x, "v") for x in (g, b, rd, v1, w, v0p, v1p, wp)],
        [(die, "c"), (f32(K, OWN), "v")],
        [vm(3, K, TC)],
    )


def solution(mesh):
    torus = Mesh(mesh.devices.reshape(2, 4, 2, 4, 2), ROW_COL)
    placed = (
        P(None, ROW, COL),
        P(ROW, COL),
        P(None, ROW_COL),
        P(ROW, COL),
        P(ROW_COL, None, None),
        P(),
        P(),
    )
    return jax.shard_map(
        body,
        mesh=torus,
        in_specs=placed,
        out_specs=(P(None, ROW, COL), P(None, ROW_COL)),
        check_vma=False,
    )
```

```python
import functools

import jax
import jax.numpy as jnp
from jax import lax
from jax.experimental import pallas as pl
from jax.experimental.pallas import tpu as pltpu
from jax.sharding import Mesh
from jax.sharding import PartitionSpec as P

ROW = ("row_0", "row_1", "row_2")
COL = ("col_0", "col_1")
ROW_COL = ("row_0", "row_1", "row_2", "col_0", "col_1")

K = 16
TR, TC = 128, 256
ER, EC = 136, 384
CELL = 32
PLANES = K + 1
PAIRS = 9
HROWS = 56
OWN = 32
NB = 4096
HI = lax.Precision.HIGHEST


def iota(shape, dim):
    return lax.broadcasted_iota(jnp.int32, shape, dim)


def where_am_i():
    i = (lax.axis_index("row_0") * 4 + lax.axis_index("row_1")) * 2 + lax.axis_index("row_2")
    j = lax.axis_index("col_0") * 2 + lax.axis_index("col_1")
    return i, j


def dot_nt(a, b):
    return lax.dot_general(
        a, b, (((1,), (1,)), ((), ())), precision=HI, preferred_element_type=jnp.float32
    )


def dot_nn(a, b):
    return jnp.dot(a, b, precision=HI, preferred_element_type=jnp.float32)


def spread(j):
    group = iota((128, EC), 1) // CELL
    cell = jnp.where(group <= 8, 8 * j + group, jnp.where(group == 11, 8 * j - 1, -5))
    return (iota((128, EC), 0) % 64 == cell).astype(jnp.float32)


def lattice_chunk(l):
    return jnp.clip(l // 2, 0, NB // 128 - 1)


def extended_rows(parts):
    body = [jnp.broadcast_to(p, (CELL, EC)) for p in parts[1:5]]
    edge = jnp.where(iota((8, EC), 0) < 4, parts[5], parts[0])
    return jnp.concatenate(body + [edge], axis=0)


def padded(scr, x):
    scr[...] = jnp.zeros_like(scr)
    scr[:, 0 : x.shape[1]] = x
    return scr[...]


def pack(vp, vd):
    lane = iota((8, 128), 1)
    hi = pltpu.roll(vp[8:16], 32, 1)
    out = jnp.where(lane < 32, vp[0:8], hi)
    out = jnp.where(lane < 64, out, pltpu.roll(vd[0:8], 64, 1))
    return jnp.where(lane < 96, out, pltpu.roll(vd[8:16], 96, 1))


def pack_package(vp):
    lane = iota((4, 128), 1)
    out = vp[0:4]
    for m in range(1, 4):
        out = jnp.where(lane // 32 == m, pltpu.roll(vp, 32 * m, 1)[4 * m : 4 * m + 4], out)
    return out


def gather_bumps(s_ref):
    at = iota((4 * TC, 128), 0)
    pick = (at // TC * 8 + at % TC // CELL == iota((4 * TC, 128), 1)).astype(jnp.float32)
    return dot_nn(s_ref[...], pick)


def down_cells(s_ref, k, z):
    for lr in range(4):
        rows = z[CELL * lr : CELL * (lr + 1)]
        s_ref[pl.ds(k, 1), TC * lr : TC * (lr + 1)] = jnp.sum(rows, axis=0, keepdims=True)


SENDS = 8


def send(msg_hbm, pay_ref, sems, pay):
    n = pay_ref.shape[0]
    for d in range(n):
        pay_ref[d] = pay
    copies = [
        pltpu.make_async_copy(pay_ref, msg_hbm.at[n * c : n * (c + 1)], sems.at[c]) for c in range(SENDS)
    ]
    for c in copies:
        c.start()
    return copies


def load_kernel(mv, b_ref, sh_ref, p_ref, msg_hbm, edge_ref, z_ref, sems):
    _, j = where_am_i()
    mv.wait(2)
    rows = [
        pltpu.make_async_copy(
            p_ref.at[:, :, 128 * t : 128 * (t + 1)],
            msg_hbm.at[:, 32 * t : 32 * (t + 1), :],
            sems.at[t],
        )
        for t in range(4)
    ]
    for c in rows:
        c.start()
    lane = iota((TR, 128), 1)
    z = jnp.zeros((TR, 128), jnp.float32)
    mv.wait(1)
    for k in [K] + list(range(K)):
        if k < K and k % 4 == 0:
            mv.wait(0, k // 4)
        src = b_ref.at[k] if k < K else sh_ref
        lo = pltpu.roll(src[:, 0:128], 3 * k, 1) if k else src[:, 0:128]
        up = pltpu.roll(src[:, 128:256], (64 + 3 * k - 125) % 128, 1)
        z = jnp.where((lane >= 3 * k) & (lane < 3 * k + 3), lo, z)
        z = jnp.where((lane >= 64 + 3 * k) & (lane < 67 + 3 * k), up, z)
        edge_ref[k, 0:8, :] = src[0:8, :]
        edge_ref[k, 8:16, :] = src[TR - 8 : TR, :]
    mv.flush(1)
    z_ref[...] = z.T
    side = lambda at, to, n: pltpu.make_async_copy(
        z_ref.at[at : at + HROWS, :], msg_hbm.at[to, 128 : 128 + HROWS, :], sems.at[n]
    )
    sides = [side(0, jnp.maximum(j - 1, 0), 4), side(64, jnp.minimum(j + 1, 7), 5)]
    for c in sides:
        c.start()
    for c in sides + rows:
        c.wait()


def start_kernel(
    mv, b_ref, sh_ref, bp_ref, m_ref, node_ref, cond_ref,
    msg_hbm, cm_ref, v0p_ref, bump_ref,
    a_ref, s_ref, t_ref, w_ref, pad_ref, pay_ref, sems,
):
    i, j = where_am_i()
    for n in (4, 5):
        mv.wait(n)
    a_ref[...] = jnp.zeros_like(a_ref)
    ln = iota((1, 128), 1)
    for lr in range(6):
        l = 4 * i + lr - 1
        chunk = lattice_chunk(l)
        ok = (ln // 64 == l % 2) & (l >= 0) & (l < 64)
        nd = node_ref[pl.ds(chunk, 1), :]
        a_ref[lr : lr + 1, :] = jnp.where(ok, nd // 2048 - CELL * l, 0).astype(jnp.float32)
        a_ref[8 + lr : 9 + lr, :] = jnp.where(ok, nd % 2048 - CELL * (ln % 64), 0).astype(jnp.float32)
        a_ref[16 + lr : 17 + lr, :] = jnp.where(ok, cond_ref[pl.ds(chunk, 1), :], 0.0)
    wide = dot_nn(a_ref[...], spread(j))
    maps = [extended_rows([wide[8 * n + lr : 8 * n + lr + 1] for lr in range(6)]) for n in range(3)]
    row = iota((ER, EC), 0)
    here = jnp.where(row < TR, row % CELL, jnp.where(row < TR + 4, row - TR, row - TR + 24))
    cols = iota((ER, EC), 1) % CELL
    hit = (maps[0].astype(jnp.int32) == here) & (maps[1].astype(jnp.int32) == cols)
    cm = jnp.where(hit, maps[2], 0.0)
    cm_ref[...] = cm
    mv.flush(1)
    mv.wait(1)
    here = cm[0:TR, 0:TC]
    rd = 1.0 / (4.0 + sh_ref[...] + here)
    at_bump = jnp.where(here > 0.0, rd, 0.0)
    row, col = iota((TR, TC), 0), iota((TR, TC), 1)
    w_ref[0] = rd
    w_ref[1] = at_bump
    for n, inside in enumerate((row > 0, row < TR - 1, col > 0, col < TC - 1)):
        w_ref[2 + n] = jnp.where(inside, at_bump, 0.0)

    def one(k, c):
        x = b_ref[k] * w_ref[0]
        at = b_ref[k] * w_ref[1]
        down_cells(s_ref, k, at)
        near = pltpu.roll(x, 1, 0) * w_ref[2] + pltpu.roll(x, TR - 1, 0) * w_ref[3]
        near = near + pltpu.roll(x, 1, 1) * w_ref[4] + pltpu.roll(x, TC - 1, 1) * w_ref[5]
        down_cells(t_ref, k, at - near)
        return c

    mv.wait(0)
    lax.fori_loop(0, K, one, 0)
    t_ref[K : K + 8, :] = jnp.zeros((8, 4 * TC), jnp.float32)
    down_cells(t_ref, K, here)
    down_cells(t_ref, K + 1, here * rd)
    bump_ref[...] = gather_bumps(t_ref)
    mv.flush(3)
    mv.wait(2)
    mv.wait(3)
    v0p = padded(pad_ref, dot_nt(bp_ref[...], m_ref[0]))
    v0p_ref[...] = v0p
    mv.flush(2)
    for c in send(msg_hbm, pay_ref, sems, pack(v0p, gather_bumps(s_ref))):
        c.wait()


def columns_kernel(mv, g1_ref, edge_ref, w_ref, up_ref, dn_ref, y_ref, ext_ref):
    _, j = where_am_i()
    y_ref[...] = jnp.zeros_like(y_ref)

    @pl.when(j < 7)
    def _():
        y_ref[0:HROWS, :] = g1_ref[jnp.minimum(j + 1, 7), 128 : 128 + HROWS, :]

    @pl.when(j > 0)
    def _():
        y_ref[64 : 64 + HROWS, :] = g1_ref[jnp.maximum(j - 1, 0), 128 : 128 + HROWS, :]

    yt = y_ref[...].T
    lane = iota((TR, 128), 1)
    for k in range(PLANES):
        right = pltpu.roll(yt, (128 - 3 * k) % 128, 1) if k else yt
        left = pltpu.roll(yt, (61 - 3 * k) % 128, 1) if (61 - 3 * k) % 128 else yt
        w_ref[k] = jnp.where(lane < 3, right, jnp.where(lane >= 125, left, 0.0))
    first = iota((8, EC), 0) < 4
    mv.wait(1)
    for k in range(PLANES):
        for side in range(2):
            ext_ref[side, k, :, 0:TC] = edge_ref[k, 8 * side : 8 * side + 8, :]
            ext_ref[side, k, :, TC:EC] = w_ref[k, (TR - 8) * side : (TR - 8) * side + 8, :]
    for p in range(PAIRS):
        q = min(p + PAIRS, PLANES - 1)
        up_ref[p] = jnp.where(first, ext_ref[0, p], pltpu.roll(ext_ref[0, q], 4, 0))
        dn_ref[p] = jnp.where(first, pltpu.roll(ext_ref[1, p], 4, 0), ext_ref[1, q])


def whole_plane(xs_ref, main, w_ref, grp_ref, k):
    xs_ref[0:TR, 0:TC] = main
    xs_ref[0:TR, TC:EC] = w_ref[k]
    xs_ref[TR:ER, :] = grp_ref[k]
    return xs_ref[...]


def package_all(g_ref, v_ref):
    lane = iota((8, 128), 1) // 32

    def one(c, carry):
        lo = jnp.zeros((8, 128), jnp.float32)
        hi = jnp.zeros((8, 128), jnp.float32)
        for m in range(4):
            x = g_ref[4 * c + m]
            lo = jnp.where(lane == m, pltpu.roll(x, 32 * m, 1) if m else x, lo)
            hi = jnp.where(lane == m, pltpu.roll(x, (32 * m - 32) % 128, 1) if m != 1 else x, hi)
        at = pl.ds(pl.multiple_of(128 * c, 128), 128)
        v_ref[0:8, at] = lo
        v_ref[8:16, at] = hi
        return carry

    lax.fori_loop(0, NB // 128, one, 0, unroll=16)


def package_only(g_ref, v_ref):
    lane = iota((4, 128), 1) // 32

    def one(c, carry):
        xs = [g_ref[4 * c + d] for d in range(4)]
        at = pl.ds(pl.multiple_of(128 * c, 128), 128)
        for m in range(4):
            out = xs[m]
            for d in range(4):
                if d != m:
                    out = jnp.where(lane == d, pltpu.roll(xs[d], (32 * (d - m)) % 128, 1), out)
            v_ref[4 * m : 4 * m + 4, at] = out
        return carry

    lax.fori_loop(0, NB // 128, one, 0, unroll=16)


def own_die(g_ref, i, j):
    lane = iota((8, 128), 1)
    halves = []
    for h in range(2):
        out = jnp.zeros((8, 128), jnp.float32)
        for m in range(4):
            x = g_ref[8 * i + 4 * (j % 2) + m]
            shift = 8 * m - (64 + 32 * h + 8 * (j // 2)) + 128
            x = pltpu.roll(x, shift % 128, 1)
            out = jnp.where((lane >= 8 * m) & (lane < 8 * m + 8), x, out)
        halves.append(out)
    return jnp.concatenate(halves, axis=0)


def own_conductance(cond_ref, i, j):
    q = 8 * i + j
    row = cond_ref[pl.ds(q // 4, 1), :]
    return pltpu.roll(row, (128 - 32 * (q % 4)) % 128, 1)


def around(v_ref, x_ref, i):
    ln = iota((K, 128), 1)
    for lr in range(6):
        l = 4 * i + lr - 1
        at = pl.ds(pl.multiple_of(128 * lattice_chunk(l), 128), 128)
        x_ref[K * lr : K * (lr + 1), :] = jnp.where(ln // 64 == l % 2, v_ref[:, at], 0.0)


def coupled(e_ref, k):
    return extended_rows([e_ref[pl.ds(K * lr + k, 1), :] for lr in range(6)])


def beside(x):
    out = pltpu.roll(x, 1, 0) + pltpu.roll(x, ER - 1, 0)
    return out + pltpu.roll(x, 1, 1) + pltpu.roll(x, EC - 1, 1)


def add_dot(r_ref, at, x):
    s = jnp.sum(x, axis=0, keepdims=True)
    r_ref[pl.ds(at, 1), :] = s[:, 0:128] + s[:, 128:256]


def tile(x):
    return x[0:TR, 0:TC]


def edges_kernel(
    mv, sh_ref, w_ref, bot_ref, top_ref, cm_ref, g1_ref, inner_ref,
    w_hbm, grp_ref, bump_ref, pm_ref,
    s_ref, t_ref, sem,
):
    keep = pltpu.make_async_copy(w_ref, w_hbm, sem.at[0])
    keep.start()
    for d in range(8):
        for t in range(4):
            c = 4 * d + t
            pm_ref[:, 128 * c : 128 * (c + 1)] = g1_ref[d, 32 * t : 32 * (t + 1), :]
    first = iota((8, EC), 0) < 4
    for p in range(PAIRS):
        bot, top = bot_ref[p], top_ref[p]
        grp_ref[p] = jnp.where(first, bot, pltpu.roll(top, 4, 0))
        if p + PAIRS < PLANES:
            grp_ref[p + PAIRS] = jnp.where(first, pltpu.roll(bot, 4, 0), top)
    mv.flush(1)
    for n in (0, 4, 6):
        mv.wait(n)
    inverse = lambda sh, cm: jnp.where(sh > 0.0, 1.0 / (4.0 + sh + cm), 0.0)
    cm = tile(cm_ref)
    at_bump = jnp.where(cm > 0.0, inverse(sh_ref[...], cm), 0.0)
    ends = inverse(grp_ref[K], cm_ref[TR:ER, :])
    above = ends[7:8, 0:TC] * at_bump[0:1]
    below = ends[0:1, 0:TC] * at_bump[TR - 1 : TR]
    lane = iota((TR, 128), 1)
    sides = jnp.where(lane == 0, pltpu.roll(at_bump[:, 128:256], 1, 1), 0.0)
    sides = jnp.where(lane == 127, pltpu.roll(at_bump[:, 0:128], 127, 1), sides)
    sides = sides * inverse(w_ref[K], cm_ref[0:TR, TC:EC])
    s_ref[...] = jnp.zeros_like(s_ref)
    for k in range(K):
        s_ref[k : k + 1, 0:TC] = grp_ref[k, 7:8, 0:TC] * above
        s_ref[k : k + 1, 3 * TC : 4 * TC] = grp_ref[k, 0:1, 0:TC] * below
        z = w_ref[k] * sides
        for lr in range(4):
            t_ref[k : k + 1, 128 * lr : 128 * (lr + 1)] = jnp.sum(
                z[CELL * lr : CELL * (lr + 1)], axis=0, keepdims=True
            )
    at, to = iota((512, 128), 0), iota((512, 128), 1)
    right = (at % 128 == 0) & (to == at // 128 * 8 + 7)
    left = (at % 128 == 127) & (to == at // 128 * 8)
    halo = gather_bumps(s_ref) + dot_nn(t_ref[...], (left | right).astype(jnp.float32))
    bump_ref[0:K, :] = inner_ref[0:K, :] - halo
    bump_ref[K:, :] = inner_ref[K:, :]
    mv.flush(2)
    keep.wait()


def package_kernel(
    step, mv, g_ref, pm_ref, m_ref, cond_ref, bump_ref, const_ref, vp_ref,
    out_ref, vd_ref, y_ref, x_ref, msg_hbm,
    v_ref, pad_ref, pay_ref, sems,
):
    i, j = where_am_i()
    package_all(g_ref, v_ref)
    for n in range(1, 7):
        if n in mv.ins:
            mv.wait(n)
    vp = vp_ref[...]
    y = padded(pad_ref, dot_nt(v_ref[...], pm_ref[...]))
    y = y + own_conductance(cond_ref, i, j) * (vp - own_die(g_ref, i, j))
    y = jnp.where(iota((K, 128), 1) < OWN, y, 0.0)
    out = padded(pad_ref, dot_nt(y[:, 0:OWN], m_ref[0]))
    if step == 2:
        out = out - vp
    vd = bump_ref[0:K, :] - const_ref[K + 1 : K + 2, :] * at_tile(v_ref, i, j)
    sent = send(msg_hbm, pay_ref, sems, pack(out, vd) if step == 1 else pack_package(out))
    y_ref[...] = y
    out_ref[...] = out
    vd_ref[...] = vd
    around(v_ref, x_ref, i)
    for n in range(4):
        mv.flush(n)
    for c in sent:
        c.wait()


def at_tile(v_ref, i, j):
    ln = iota((K, 128), 1)
    out = jnp.zeros((K, 128), jnp.float32)
    for lr in range(4):
        l = 4 * i + lr
        at = pl.ds(pl.multiple_of(128 * lattice_chunk(l), 128), 128)
        x = pltpu.roll(v_ref[:, at], (8 * lr - 64 * (l % 2) - 8 * j + 256) % 128, 1)
        out = jnp.where((ln >= 8 * lr) & (ln < 8 * lr + 8), x, out)
    return out


def second_kernel(
    mv, b_ref, sh_ref, w_ref, grp_ref, cm_ref, x_ref, bp_ref, v0p_ref, v1p_ref, y1_ref,
    v1_ref, bump_ref, r_ref, rd_ref, dg_ref, cr_ref, next_ref,
    e_ref, s_ref, pad_ref, xs_ref,
):
    i, j = where_am_i()
    for n in range(1, 10):
        mv.wait(n)
    sh = whole_plane(xs_ref, sh_ref[...], w_ref, grp_ref, K)
    cm = cm_ref[...]
    rd = jnp.where(sh > 0.0, 1.0 / (4.0 + sh + cm), 0.0)
    rd_ref[...] = rd
    cr_ref[...] = cm * rd
    dg_ref[...] = 4.0 + tile(sh) + tile(cm)
    for n in (3, 4, 5):
        mv.flush(n)
    e_ref[...] = dot_nn(x_ref[...], spread(j))

    def one(k, c):
        rd, dg = rd_ref[...], dg_ref[...]
        x0 = whole_plane(xs_ref, b_ref[k], w_ref, grp_ref, k) * rd
        x1 = x0 - (beside(x0) * rd + cr_ref[...] * coupled(e_ref, k))
        v1_ref[k] = tile(x1)
        near = -beside(x1) * rd
        next_ref[k] = near
        down_cells(s_ref, k, jnp.where(tile(cr_ref) > 0.0, tile(near), 0.0))
        a, b = tile(x0), tile(x1)
        add_dot(r_ref, k, dg * a * a)
        add_dot(r_ref, K + k, dg * a * b)
        add_dot(r_ref, 2 * K + k, dg * b * b)
        return c

    for c in range(CHUNKS):
        mv.wait(0, c)
        lax.fori_loop(4 * c, 4 * c + 4, one, 0)
        mv.flush(0, c)
        mv.flush(6, c)
    bump_ref[...] = gather_bumps(s_ref)
    v0p, v1p, y1 = v0p_ref[...], v1p_ref[...], y1_ref[...]
    bp = padded(pad_ref, bp_ref[...])
    r_ref[0:K, :] += v0p * bp
    r_ref[K : 2 * K, :] += v0p * y1
    r_ref[2 * K : 3 * K, :] += v1p * y1
    mv.flush(2)


def third_kernel(
    mv, next_ref, v1_ref, rd_ref, dg_ref, cr_ref, x_ref, wp_ref, y1_ref, y2_ref, ra_ref,
    wt_ref, r_ref,
    e_ref,
):
    i, j = where_am_i()
    for n in range(2, 10):
        mv.wait(n)
    e_ref[...] = dot_nn(x_ref[...], spread(j))
    r_ref[6 * K :, :] = jnp.zeros((2 * K, 128), jnp.float32)
    r_ref[0 : 3 * K, :] = ra_ref[...]

    def one(k, c):
        dg = dg_ref[...]
        w = next_ref[k] - cr_ref[...] * coupled(e_ref, k)
        a, b = v1_ref[k], tile(w)
        wt_ref[k] = b
        add_dot(r_ref, 3 * K + k, dg * a * b)
        add_dot(r_ref, 4 * K + k, dg * b * b)
        add_dot(r_ref, 5 * K + k, dg * b * (b - tile(beside(w)) * tile(rd_ref)))
        return c

    for c in range(CHUNKS):
        mv.wait(0, c)
        mv.wait(1, c)
        lax.fori_loop(4 * c, 4 * c + 4, one, 0)
        mv.flush(0, c)
    wp, y1, y2 = wp_ref[...], y1_ref[...], y2_ref[...]
    r_ref[3 * K : 4 * K, :] += wp * y1
    r_ref[4 * K : 5 * K, :] += wp * (y2 - y1)


def fourth_kernel(
    mv, g_ref, pm_ref, cond_ref, const_ref, wp_ref, wd_ref, ra_ref, v1_hbm, w_hbm,
    msg_ref, v1_ref, w_ref,
    v_ref, pad_ref, r_ref, sems,
):
    i, j = where_am_i()
    loads = [
        pltpu.make_async_copy(v1_hbm, v1_ref, sems.at[0]),
        pltpu.make_async_copy(w_hbm, w_ref, sems.at[1]),
    ]
    for c in loads:
        c.start()
    package_only(g_ref, v_ref)
    for n in range(2, 6):
        mv.wait(n)
    wp = wp_ref[...]
    y = padded(pad_ref, dot_nt(v_ref[...], pm_ref[...])) + own_conductance(cond_ref, i, j) * wp
    y = jnp.where(iota((K, 128), 1) < OWN, y, 0.0)
    r_ref[...] = ra_ref[...]
    both = const_ref[K : K + 1, :] * wd_ref[...] * at_tile(v_ref, i, j)
    r_ref[5 * K : 6 * K, :] += wp * y - 2.0 * both
    sums = dot_nt(jnp.ones((8, 128), jnp.float32), r_ref[...])

    def one(d, c):
        msg_ref[d] = sums[0:1]
        return c

    lax.fori_loop(0, msg_ref.shape[0], one, 0, unroll=8)
    for c in loads:
        c.wait()


def last_kernel(
    mv, g_ref, b_ref, rd_ref, v1_ref, v2_ref, v0p_ref, v1p_ref, v2p_ref,
    xd_ref, xp_ref, c_ref,
):
    total = jnp.sum(g_ref[...], axis=0)
    total = jnp.broadcast_to(total, (8, 128))
    m = [pltpu.roll(total, (128 - K * n) % 128, 1) if n else total for n in range(6)]
    g00, g01, g02, g11, g12, g22 = m[1], m[2], m[3], m[2] + m[3], m[3] + m[4], m[5]
    f1, f2 = g01 / g00, g02 / g00
    a11, a12, h1 = g11 - f1 * g01, g12 - f1 * g02, g00 - f1 * m[0]
    a22, h2 = g22 - f2 * g02, g01 - g00 - f2 * m[0]
    f3 = a12 / a11
    c2 = (h2 - f3 * h1) / (a22 - f3 * a12)
    c1 = (h1 - a12 * c2) / a11
    c0 = (m[0] - g01 * c1 - g02 * c2) / g00
    rd = tile(rd_ref)
    at = iota((K, 128), 0) == iota((K, 128), 1)
    cols = []
    for n, c in enumerate((c0, c1, c2)):
        col = jnp.sum(jnp.where(at, c[0:1], 0.0), axis=1, keepdims=True)
        cols.append(col)
        c_ref[n] = jnp.broadcast_to(col, (K, TC))
    xp = cols[0] * v0p_ref[...] + cols[1] * v1p_ref[...] + cols[2] * v2p_ref[...]
    xp_ref[...] = xp[:, 0:OWN]

    def one(k, carry):
        c0, c1, c2 = (c_ref[n, pl.ds(k, 1), :] for n in range(3))
        xd_ref[k] = (c0 * b_ref[k]) * rd + c1 * v1_ref[k] + c2 * v2_ref[k]
        return carry

    for c in range(CHUNKS):
        lax.fori_loop(4 * c, 4 * c + 4, one, 0)
        mv.flush(0, c)


def f32(*shape):
    return jax.ShapeDtypeStruct(shape, jnp.float32)


def vm(*shape):
    return pltpu.VMEM(shape, jnp.float32)


CHUNKS = 4


class Moves:
    def __init__(self):
        self.ins, self.outs, self.pending = {}, {}, []

    def wait(self, n, chunk=None):
        for c in [chunk] if chunk is not None else range(len(self.ins[n])):
            self.ins[n][c].wait()
            self.ins[n][c] = None

    def flush(self, n, chunk=None):
        for c in [chunk] if chunk is not None else range(len(self.outs[n])):
            self.outs[n][c].start()
            self.pending.append(self.outs[n][c])


def parts(ref, mode):
    if mode == "h":
        return [ref]
    step = ref.shape[0] // CHUNKS
    return [ref.at[step * c : step * (c + 1)] for c in range(CHUNKS)]


def call(kernel, ins, outs, scratch, limit=14, **kw):
    imode, omode = [m for _, m in ins], [m for _, m in outs]
    moved = [jax.ShapeDtypeStruct(x.shape, x.dtype) for x, m in ins + outs if m in "hc"]
    count = sum({"h": 1, "c": CHUNKS}.get(m, 0) for m in imode + omode)

    def wrapped(*refs):
        ni, no, nm = len(ins), len(outs), len(moved)
        hbm, bufs, sems, own = refs[: ni + no], list(refs[ni + no :][:nm]), refs[ni + no + nm], refs[ni + no + nm + 1 :]
        mv, given, sem = Moves(), [], 0
        for n, (ref, mode) in enumerate(zip(hbm, imode + omode)):
            if mode not in "hc":
                given.append(ref)
                continue
            buf = bufs.pop(0)
            given.append(buf)
            copies = []
            for x, y in zip(parts(ref, mode), parts(buf, mode)):
                x, y = (x, y) if n < ni else (y, x)
                copies.append(pltpu.make_async_copy(x, y, sems.at[sem]))
                sem += 1
            (mv.ins if n < ni else mv.outs)[n if n < ni else n - ni] = copies
        for copies in sorted(mv.ins.values(), key=len):
            for c in copies:
                c.start()
        kernel(mv, *given, *own)
        for copies in mv.ins.values():
            assert all(c is None for c in copies)
        for c in mv.pending:
            c.wait()

    space = lambda m: pl.BlockSpec(memory_space=pltpu.VMEM if m == "v" else pltpu.HBM)
    return pl.pallas_call(
        wrapped,
        out_shape=tuple(x if m == "v" else pltpu.HBM(x.shape, x.dtype) for x, m in outs),
        in_specs=[space(m) for m in imode],
        out_specs=tuple(space(m) for m in omode),
        scratch_shapes=[pltpu.VMEM(x.shape, x.dtype) for x in moved]
        + [pltpu.SemaphoreType.DMA((max(count, 1),))] + scratch,
        compiler_params=pltpu.CompilerParams(vmem_limit_bytes=limit << 20),
        name=getattr(kernel, "func", kernel).__name__,
        **kw,
    )(*[x if m == "v" else pltpu.with_memory_space_constraint(x, pltpu.HBM) for x, m in ins])


def swapped(x, axes):
    return lax.all_to_all(x, axes, 0, 0, tiled=True)


def body(
    die_current, die_shunt, pkg_current, pkg_matrix, pkg_block_inv, bump_node, bump_conductance
):
    nodes = bump_node.reshape(NB // 128, 128)
    cond = bump_conductance.reshape(NB // 128, 128)
    b, sh, bp, m = die_current, die_shunt, pkg_current, pkg_block_inv
    gathered, small, ext, die = f32(128, 8, 128), f32(K, 128), f32(K, ER, EC), f32(K, TR, TC)
    lattice = f32(6 * K, 128)
    payload = [vm(128 // SENDS, 8, 128), pltpu.SemaphoreType.DMA((SENDS,))]
    alone = [vm(128 // SENDS, 4, 128)] + payload[1:]
    msg1, edge = call(
        load_kernel,
        [(b, "c"), (sh, "h"), (pkg_matrix.reshape(8, OWN, 512), "h")],
        [(f32(8, 128 + HROWS, 128), "r"), (f32(PLANES, 16, TC), "h")],
        [vm(128, 128), pltpu.SemaphoreType.DMA((6,))],
    )
    g1 = swapped(msg1, COL)
    msg, cm, v0p, bump1 = call(
        start_kernel,
        [(b, "h"), (sh, "h"), (bp, "h"), (m, "h"), (nodes, "h"), (cond, "h")],
        [(gathered, "r"), (f32(ER, EC), "h"), (small, "h"), (f32(K + 8, 128), "h")],
        [vm(24, 128), vm(K, 4 * TC), vm(K + 8, 4 * TC), vm(6, TR, TC), vm(K, 128)] + payload,
    )
    g = swapped(msg, ROW_COL)
    side, up, dn = call(
        columns_kernel,
        [(g1, "v"), (edge, "h")],
        [(f32(PLANES, TR, 128), "v"), (f32(PAIRS, 8, EC), "v"), (f32(PAIRS, 8, EC), "v")],
        [vm(128, 128), vm(2, PLANES, 8, EC)],
    )
    n = lax.axis_size(ROW)
    bot = lax.ppermute(up, ROW, [(r + 1, r) for r in range(n - 1)])
    top = lax.ppermute(dn, ROW, [(r, r + 1) for r in range(n - 1)])
    side, grp, bump1, pm = call(
        edges_kernel,
        [(sh, "h"), (side, "v"), (bot, "v"), (top, "v"), (cm, "h"), (g1, "v"), (bump1, "h")],
        [
            (f32(PLANES, TR, 128), "r"), (f32(PLANES, 8, EC), "h"), (f32(K + 8, 128), "h"),
            (f32(OWN, NB), "v"),
        ],
        [vm(K, 4 * TC), vm(K, 512), pltpu.SemaphoreType.DMA((1,))],
    )
    step = [vm(K, NB), vm(K, 128)]
    results = [(small, "h"), (small, "h"), (small, "h"), (lattice, "h")]
    v1p, _, y1, near, msg = call(
        functools.partial(package_kernel, 1),
        [(g, "v"), (pm, "v"), (m, "h"), (cond, "h"), (bump1, "h"), (bump1, "h"), (v0p, "h")],
        results + [(gathered, "r")],
        step + payload,
    )
    g = swapped(msg, ROW_COL)
    v1, bump2, r, rd, dg, cr, near1 = call(
        second_kernel,
        [(b, "c")] + [(x, "h") for x in (sh, side, grp, cm, near, bp, v0p, v1p, y1)],
        [
            (die, "c"), (small, "v"), (f32(3 * K, 128), "h"), (f32(ER, EC), "h"),
            (f32(TR, TC), "h"), (f32(ER, EC), "h"), (ext, "c"),
        ],
        [vm(6 * K, EC), vm(K, 4 * TC), vm(K, 128), vm(ER, EC)],
    )
    wp, wd, y2, near, msg = call(
        functools.partial(package_kernel, 2),
        [(g, "v"), (pm, "v"), (m, "h"), (cond, "h"), (bump2, "v"), (bump1, "h"), (v1p, "h")],
        results + [(f32(128, 4, 128), "r")],
        step + alone,
    )
    g = swapped(msg, ROW_COL)
    w, r = call(
        third_kernel,
        [(near1, "c"), (v1, "c")] + [(x, "h") for x in (rd, dg, cr, near, wp, y1, y2, r)],
        [(die, "c"), (f32(128, 128), "v")],
        [vm(6 * K, EC)],
    )
    msg, v1, w = call(
        fourth_kernel,
        [(g, "v"), (pm, "v")] + [(x, "h") for x in (cond, bump1, wp, wd)] + [(r, "v"), (v1, "r"), (w, "r")],
        [(f32(128, 1, 128), "v"), (die, "v"), (die, "v")],
        [vm(K, NB), vm(K, 128), vm(128, 128), pltpu.SemaphoreType.DMA((2,))],
    )
    g = swapped(msg, ROW_COL)
    return call(
        last_kernel,
        [(x, "v") for x in (g, b, rd, v1, w, v0p, v1p, wp)],
        [(die, "c"), (f32(K, OWN), "v")],
        [vm(3, K, TC)],
    )


def solution(mesh):
    torus = Mesh(mesh.devices.reshape(2, 4, 2, 4, 2), ROW_COL)
    placed = (
        P(None, ROW, COL),
        P(ROW, COL),
        P(None, ROW_COL),
        P(ROW, COL),
        P(ROW_COL, None, None),
        P(),
        P(),
    )
    return jax.shard_map(
        body,
        mesh=torus,
        in_specs=placed,
        out_specs=(P(None, ROW, COL), P(None, ROW_COL)),
        check_vma=False,
    )
```
